32 devices in a mesh: exp: 8 (over z, x), dat: 4 (over y, core).
Axes of the slice: x: 2, y: 2, z: 4, core: 2. Of those that a mesh axis runs over, the one named last changes fastest.
Arguments:
- tokens: bfloat16 [4096, 1024], P(('exp', 'dat')), may hold values from -6 to 6
- norm_gain: float32 [1024], replicated, may hold values from 0.25 to 1.75
- router_weight: bfloat16 [1024, 32], P(None, 'exp'), may hold values from -0.1875 to 0.1875
- inner_weight: bfloat16 [32, 1024, 4096], P('exp', None, 'dat'), may hold values from -0.1875 to 0.1875
- outer_weight: bfloat16 [32, 4096, 1024], P('exp', 'dat'), may hold values from -0.09375 to 0.09375
- slot_tokens: int32 [32, 256], P('exp', 'dat'), may hold values from 0 to 4095, as said below
- slot_ids: int32 [4096, 2], P(('exp', 'dat')), may hold values from 0 to 8191, as said below
Outputs:
- mixed: bfloat16 [4096, 1024], P(('exp', 'dat'))
The draws below stay inside these ranges and needn't reach their ends.
Inputs may be any that keep to these rules, and one draw needn't show every extreme that they name: `slot_tokens`: column c of an expert names only tokens of the devices whose dat index is c // 64; one expert names no token twice. The 256 slots of the experts of one exp index in one dat group name tokens of any one device at most 96 times, exactly 96 times for some devices, and no times for some. Every token is named by exactly 2 slots. slot_ids[t] holds the two slots e * 256 + c with slot_tokens[e, c] = t, the smaller first.
All inputs are finite; a program needn't handle non-finite values.
Results may differ from the reference program's by a relative error of at most 0.0085.
Values may be sent and summed in bfloat16 or wider, within the bound.
A program may use at most 64 MiB of HBM per device.

```python
import jax
import jax.numpy as jnp
from jax import lax

D = 1024
FF = 4096
E_DEV = 4
TOK_DEV = 128
E = 32
C_DAT = 64
CAP = 256
TOKENS = 4096
N_EXP = 8
N_DAT = 4


def build_routes(key):
    base = jax.random.fold_in(key, 7)
    groups = N_DAT
    owners = N_EXP
    tok_rows = TOK_DEV
    spread = E_DEV * C_DAT
    average = 2 * TOK_DEV // N_EXP
    ranking = jnp.arange(owners, dtype=jnp.int32)
    profile = jnp.where(ranking < owners // 8, 3 * average, jnp.where(ranking < 3 * owners // 4, average, 0)).astype(jnp.int32)
    key_shift, key_slot, key_token = jax.random.split(base, 3)
    shifts = jax.vmap(lambda subkey: jax.random.permutation(subkey, owners))(jax.random.split(key_shift, groups)).astype(jnp.int32)
    counts = profile[(ranking[None, None, :] + shifts[:, :, None]) % owners]
    after_dev = jnp.cumsum(counts, axis=1)
    start_dev = after_dev - counts
    after_own = jnp.cumsum(counts, axis=2)
    start_own = after_own - counts
    orders = jax.vmap(lambda subkey: jax.random.permutation(subkey, spread))(jax.random.split(key_slot, groups * owners)).reshape(groups, owners, spread).astype(jnp.int32)
    circuits = jax.vmap(lambda subkey: jax.random.permutation(subkey, tok_rows))(jax.random.split(key_token, groups * owners)).reshape(groups, owners, tok_rows).astype(jnp.int32)
    owner_of = jnp.sum((after_own[:, :, None, :] <= orders[:, :, :, None]).astype(jnp.int32), axis=-1)
    within = orders - jnp.take_along_axis(start_own, owner_of, axis=2)
    position = jnp.take_along_axis(start_dev, owner_of, axis=2) + within
    flat_index = (owner_of * tok_rows + position % tok_rows).reshape(groups, owners * spread)
    local_token = jnp.take_along_axis(circuits.reshape(groups, owners * tok_rows), flat_index, axis=1).reshape(groups, owners, spread)
    group_index = jnp.arange(groups, dtype=jnp.int32)[:, None, None]
    token_id = (owner_of * groups + group_index) * tok_rows + local_token
    slot_tokens = token_id.reshape(groups, owners, E_DEV, C_DAT).transpose(1, 2, 0, 3).reshape(owners * E_DEV, groups * C_DAT)
    steps_seq = jnp.arange(2 * tok_rows, dtype=jnp.int32)
    after_by_owner = after_dev.transpose(0, 2, 1)
    device_of = jnp.sum((after_by_owner[:, :, None, :] <= steps_seq[None, None, :, None]).astype(jnp.int32), axis=-1)
    within_dev = steps_seq[None, None, :] - jnp.take_along_axis(start_dev.transpose(0, 2, 1), device_of, axis=2)
    sorted_pos = jnp.take_along_axis(start_own.transpose(0, 2, 1), device_of, axis=2) + within_dev
    inverse = jnp.argsort(orders, axis=-1).astype(jnp.int32)
    flat_slot = (device_of * spread + sorted_pos).reshape(groups, owners * 2 * tok_rows)
    slot_pos = jnp.take_along_axis(inverse.reshape(groups, owners * spread), flat_slot, axis=1).reshape(groups, owners, 2 * tok_rows)
    slot_global = (device_of * E_DEV + slot_pos // C_DAT) * CAP + group_index * C_DAT + slot_pos % C_DAT
    token_place = jnp.argsort(circuits, axis=-1).astype(jnp.int32)
    earlier_id = jnp.take_along_axis(slot_global, token_place, axis=2)
    later_id = jnp.take_along_axis(slot_global, token_place + tok_rows, axis=2)
    paired = jnp.stack([jnp.minimum(earlier_id, later_id), jnp.maximum(earlier_id, later_id)], axis=-1)
    slot_ids = paired.transpose(1, 0, 2, 3).reshape(owners * groups * tok_rows, 2)
    return (slot_tokens.astype(jnp.int32), slot_ids.astype(jnp.int32))


def draw_slot_tokens(key, part):
    return build_routes(key)[0]


def draw_slot_ids(key, part):
    return build_routes(key)[1]


def shard_levels(rng, extent, cuts, smallest, high):
    factor_of, own = 1.0, jax.random.fold_in(rng, 6)
    for dim, blocks in cuts:
        draws = jnp.exp(jax.random.uniform(jax.random.fold_in(own, dim), (blocks,), jnp.float32, smallest / len(cuts), high / len(cuts)))
        factor_of = factor_of * jnp.repeat(draws, extent[dim] // blocks).reshape([-1 if axis == dim else 1 for axis in range(len(extent))])
    return factor_of


def normal_values(own_key, extent, width, bound, cuts=(), kind=jnp.bfloat16):
    values = width * jax.random.normal(own_key, extent, jnp.float32)
    if cuts:
        values = values * shard_levels(own_key, extent, cuts, -0.22, 0.18)
    return jnp.clip(values, -bound, bound).astype(kind)


def setup_inputs(seed: int = 0) -> dict:
    keys = jax.random.split(jax.random.key(seed), 8)
    tokens = normal_values(keys[0], (TOKENS, D), 1.0, 6.0, ((0, 32),))
    norm_gain = jnp.clip(1.0 + 0.15 * jax.random.normal(keys[1], (D,), jnp.float32), 0.25, 1.75)
    router_weight = normal_values(keys[2], (D, E), D ** -0.5, 0.1875, ((1, 8),))
    inner_weight = normal_values(keys[3], (E, D, FF), D ** -0.5, 0.1875, ((0, 8), (2, 4)))
    outer_weight = normal_values(keys[4], (E, FF, D), FF ** -0.5, 0.09375, ((0, 8), (1, 4)))
    slot_tokens = draw_slot_tokens(jax.random.fold_in(keys[7], 71), 0)
    slot_ids = draw_slot_ids(jax.random.fold_in(keys[7], 71), 0)
    return dict(tokens=tokens, norm_gain=norm_gain, router_weight=router_weight, inner_weight=inner_weight, outer_weight=outer_weight, slot_tokens=slot_tokens, slot_ids=slot_ids)


EPSILON = 1e-06

def reference(tokens, norm_gain, router_weight, inner_weight, outer_weight, slot_tokens, slot_ids):
    values = tokens.astype(jnp.float32)
    scale = lax.rsqrt(lax.optimization_barrier(jnp.mean(values * values, axis=-1, keepdims=True)) + EPSILON)
    normed = (values * scale * norm_gain.astype(jnp.float32)).astype(jnp.bfloat16)
    slot_rows = jnp.take(normed, slot_tokens, axis=0)
    gate_score = jax.nn.sigmoid(jnp.einsum('ecd,de->ec', slot_rows.astype(jnp.float32), router_weight.astype(jnp.float32)))
    capacity = slot_tokens.shape[1]
    ff_block = FF // N_DAT

    def expert(inputs):
        block, first_weight, second_weight = inputs
        hidden = jax.nn.relu(jnp.dot(block, first_weight, preferred_element_type=jnp.float32)).astype(jnp.bfloat16)
        pieces = hidden.reshape(capacity, N_DAT, ff_block).astype(jnp.float32)
        seconds = second_weight.reshape(N_DAT, ff_block, D).astype(jnp.float32)
        partial_sums = jnp.einsum('ckf,kfd->kcd', pieces, seconds).astype(jnp.bfloat16)
        partial_sums = lax.optimization_barrier(partial_sums)
        return lax.optimization_barrier(jnp.sum(partial_sums.astype(jnp.float32), axis=0))
    expert_out = lax.map(expert, (slot_rows, inner_weight, outer_weight))
    weighted = (gate_score[:, :, None] * expert_out).astype(jnp.bfloat16).reshape(-1, D)
    chosen = jnp.take(weighted, slot_ids.reshape(-1), axis=0).reshape(slot_ids.shape[0], 2, D).astype(jnp.float32)
    combined = chosen[:, 0] + chosen[:, 1]
    return (values + combined).astype(jnp.bfloat16)
```

```python
import jax
import jax.numpy as jnp
from jax import lax
from jax.experimental import pallas as pl
from jax.experimental.pallas import tpu as pltpu
from jax.sharding import PartitionSpec as P

EPSILON = 1e-06


def normalize(tokens, norm_gain):
    values = tokens.astype(jnp.float32)
    scale = lax.rsqrt(jnp.mean(values * values, axis=-1, keepdims=True) + EPSILON)
    return (values * scale * norm_gain).astype(jnp.bfloat16)


def owner_places(slot_ids, experts_dev, capacity, bucket):
    flat_ids = slot_ids.reshape(-1)
    source = flat_ids // capacity // experts_dev
    before = (source[:, None] == source[None, :]) & (flat_ids[None, :] < flat_ids[:, None])
    ranks_in = jnp.sum(before.astype(jnp.int32), axis=1)
    return (source * bucket + ranks_in).reshape(slot_ids.shape)


def expert_places(token_ids, slot_keys, tok_rows, dat_count, bucket):
    owner_of = token_ids // (tok_rows * dat_count)
    before = (owner_of[:, None] == owner_of[None, :]) & (slot_keys[None, :] < slot_keys[:, None])
    ranks_in = jnp.sum(before.astype(jnp.int32), axis=1)
    return owner_of * bucket + ranks_in


def body(tokens, norm_gain, router_weight, inner_weight, outer_weight, slot_tokens, slot_ids):
    exp_count = lax.axis_size("exp")
    dat_count = lax.axis_size("dat")
    tok_rows, width = tokens.shape
    experts_dev, cap_dev = slot_tokens.shape
    bucket = 6 * tok_rows // exp_count
    normed = normalize(tokens, norm_gain)
    picked = slot_tokens.T.reshape(-1)
    expert_iota = lax.broadcasted_iota(jnp.int32, (cap_dev, experts_dev), 1)
    column_iota = lax.broadcasted_iota(jnp.int32, (cap_dev, experts_dev), 0)
    slot_keys = (expert_iota * cap_dev + column_iota).reshape(-1)
    senders = expert_places(picked, slot_keys, tok_rows, dat_count, bucket)
    receivers = owner_places(slot_ids, experts_dev, cap_dev * dat_count, bucket)
    lookup = jnp.any(
        lax.broadcasted_iota(jnp.int32, (exp_count * bucket, 1, 1), 0) == receivers[None], axis=2
    )
    outgoing = jnp.dot(lookup.astype(jnp.bfloat16), normed, preferred_element_type=jnp.float32)
    outgoing = outgoing.astype(jnp.bfloat16).reshape(exp_count, bucket, width)
    arrived = lax.all_to_all(outgoing, "exp", split_axis=0, concat_axis=0, tiled=True).reshape(
        exp_count * bucket, width
    )
    gathered_rows = jnp.take(arrived, senders, axis=0)
    gathered_rows = gathered_rows.reshape(cap_dev, experts_dev, width)
    gate_score = jax.nn.sigmoid(
        jnp.einsum("ced,de->ce", gathered_rows, router_weight, preferred_element_type=jnp.float32)
    )
    inner = jnp.einsum(
        "ced,edf->cef",
        lax.all_gather(gathered_rows, "dat", axis=0, tiled=True),
        inner_weight,
        preferred_element_type=jnp.float32,
    )
    hidden = jax.nn.relu(inner).astype(jnp.bfloat16)
    expert_out = lax.psum_scatter(
        jnp.einsum("cef,efd->ced", hidden, outer_weight, preferred_element_type=jnp.float32).astype(
            jnp.bfloat16
        ),
        "dat",
        scatter_dimension=0,
        tiled=True,
    ).astype(jnp.float32)
    weighted = (gate_score[:, :, None] * expert_out).astype(jnp.bfloat16).reshape(-1, width)
    placing = lax.broadcasted_iota(jnp.int32, (exp_count * bucket, 1), 0) == senders[None, :]
    returning = jnp.dot(placing.astype(jnp.bfloat16), weighted, preferred_element_type=jnp.float32)
    returning = returning.astype(jnp.bfloat16).reshape(exp_count, bucket, width)
    came_back = lax.all_to_all(returning, "exp", split_axis=0, concat_axis=0, tiled=True).reshape(
        exp_count * bucket, width
    )
    combine_table = jnp.sum(
        (
            lax.broadcasted_iota(jnp.int32, (1, 1, exp_count * bucket), 2) == receivers[:, :, None]
        ).astype(jnp.float32),
        axis=1,
    )
    combined = jnp.dot(
        combine_table.astype(jnp.bfloat16), came_back, preferred_element_type=jnp.float32
    )
    return (tokens.astype(jnp.float32) + combined).astype(jnp.bfloat16)


MESH = pl.DeviceIdType.MESH
PAIR = 2
LINE = 4
LANES = 128
PARTS = 2


def moe_kernel(
    tokens_ref, gain_ref, router_ref, ids_ref, inner_hbm, outer_hbm, out_ref,
    inner_v, outer_v, ids_all, pick_own, place_own, pick_far, place_far,
    blocks, cross, pick_send, pick_recv, swap_send, rows, sums, hidden, gate,
    parts, core_recv, y_send, y_recv, kept, give, slots_v, raw, dense, dest_send, dest_recv,
    last_send, last_recv, last_own,
    w_sem, ids_sem, x_sem, near_sem, far_sem, pick_sem, swap_sem, y_sem, c_sem, cr_sem,
    rc_sem, ry_sem, rx_sem, raw_sem, dest_sem, last_sem,
):
    chunks = blocks.shape[0]
    tok_rows = tokens_ref.shape[0]
    experts_dev, cap_dev = ids_ref.shape
    slots = experts_dev * cap_dev
    both = PAIR * tok_rows
    wide = PAIR * LANES
    pair_e = experts_dev // PARTS
    bf16, f32 = jnp.bfloat16, jnp.float32
    exp = lax.axis_index("exp")
    dat = lax.axis_index("dat")
    dat_count = lax.axis_size("dat")
    z, x = exp // PAIR, exp % PAIR
    y, c = dat // PAIR, dat % PAIR
    half = z // PAIR
    spot = z + half * (LINE - 1 - 2 * z)
    is_end = spot == 0
    is_inner = spot == 1

    def line_z(q):
        return q + half * (LINE - 1 - 2 * q)

    near = (line_z(1 - spot) * PAIR + x, dat)
    far_inner = (line_z(2) * PAIR + x, dat)
    far_end = (line_z(3) * PAIR + x, dat)
    x_peer = (exp + 1 - 2 * x, dat)
    y_peer = (exp, dat + PAIR - 2 * PAIR * y)
    c_peer = (exp, dat + 1 - 2 * c)
    sent = []

    def copy_to(src, dst, sems, where, peer):
        return pltpu.make_async_remote_copy(
            src_ref=src, dst_ref=dst, send_sem=sems.at[(0,) + where],
            recv_sem=sems.at[(1,) + where], device_id=peer, device_id_type=MESH,
        )

    def send(copy, cond=None):
        sent.append((copy, cond))
        if cond is None:
            copy.start()
        else:
            pl.when(cond)(copy.start)

    loads = []
    for e in range(experts_dev):
        loads.append(pltpu.make_async_copy(inner_hbm.at[e], inner_v.at[e], w_sem.at[0, e]))
    for e in range(experts_dev):
        loads.append(pltpu.make_async_copy(outer_hbm.at[e], outer_v.at[e], w_sem.at[1, e]))

    barrier = pltpu.get_barrier_semaphore()
    for peer in (near, far_inner, x_peer, y_peer, c_peer):
        pl.semaphore_signal(barrier, inc=1, device_id=peer, device_id_type=MESH)

    @pl.when(is_inner)
    def _():
        pl.semaphore_signal(barrier, inc=1, device_id=far_end, device_id_type=MESH)

    for load in loads:
        load.start()

    values = tokens_ref[...].astype(f32)
    scale = lax.rsqrt(jnp.mean(values * values, axis=-1, keepdims=True) + EPSILON)
    normed = values * scale * gain_ref[...]

    def split(value):
        low, high = value[..., :LANES], value[..., LANES:]
        return jnp.where(x == 0, low, high), jnp.where(x == 0, high, low)

    for k in range(chunks):
        own, other = split(normed[:, k * wide : (k + 1) * wide])
        blocks[k, spot, 0] = own.astype(bf16)
        cross[k] = other.astype(bf16)

    def one_hots(ids, side, pick, place, first):
        row = jnp.concatenate([ids[e : e + 1, :] for e in range(experts_dev)], axis=1)
        column = jnp.broadcast_to(row, (LANES, slots)).T
        lane = lax.broadcasted_iota(jnp.int32, (slots, tok_rows), 1)
        line = lax.broadcasted_iota(jnp.int32, (tok_rows, slots), 0)
        at = slice(side * slots, (side + 1) * slots)
        for q in range(first, LINE):
            for xr in range(PAIR):
                x_of = x if xr == 0 else 1 - x
                base = ((line_z(q) * PAIR + x_of) * dat_count + dat) * tok_rows
                start = ((q - first) * PAIR + xr) * tok_rows
                span = slice(start, start + tok_rows)
                pick[at, span] = (column == lane + base).astype(f32).astype(bf16)
                place[span, at] = (row == line + base).astype(f32).astype(bf16)

    one_hots(ids_ref, 0, pick_own, place_own, 0)

    pl.semaphore_wait(barrier, 5 + is_inner.astype(jnp.int32))

    def cross_copy(k):
        return copy_to(cross.at[k], blocks.at[k, spot, 1], x_sem, (k,), x_peer)

    ids_x = copy_to(ids_ref, ids_all.at[1], ids_sem, (0,), x_peer)
    ids_own = copy_to(ids_ref, ids_all.at[2], ids_sem, (1,), near)
    ids_fwd = copy_to(ids_all.at[1], ids_all.at[3], ids_sem, (2,), near)

    def near_copy(k, xr):
        return copy_to(blocks.at[k, 0, xr], blocks.at[k, 0, xr], near_sem, (k, xr), near)

    def far_copy(k, j, xr):
        return copy_to(blocks.at[k, 1 - j, xr], blocks.at[k, 2 + j, xr], far_sem, (k, j, xr), far_inner)

    def block_send(k, xr):
        send(far_copy(k, 1 - spot, xr))
        send(near_copy(k, xr), is_end)

    send(ids_x)
    send(ids_own, is_end)
    send(cross_copy(0))
    block_send(0, 0)
    for k in range(1, chunks):
        send(cross_copy(k))
        if k < chunks - 1:
            block_send(k, 0)
    ids_x.wait_recv()
    send(ids_fwd, is_end)
    one_hots(ids_all.at[1], 1, pick_own, place_own, 0)
    for k in range(chunks):
        cross_copy(k).wait_recv()
        block_send(k, 1)
        if k == 0:
            block_send(chunks - 1, 0)

    @pl.when(is_inner)
    def _():
        ids_own.wait_recv()
        ids_fwd.wait_recv()
        one_hots(ids_all.at[2], 0, pick_far, place_far, 1)
        one_hots(ids_all.at[3], 1, pick_far, place_far, 1)

    def pair(p):
        return slice(p * pair_e, (p + 1) * pair_e)

    def own_rows(k, rel, p, of_dat):
        feature = k * PAIR + (x if rel == 0 else 1 - x)
        at = pl.ds(pl.multiple_of(of_dat * cap_dev, cap_dev), cap_dev)
        return rows.at[feature, pair(p), at]

    def pick_copy(k, xr, p):
        return copy_to(
            pick_send.at[k, xr, pair(p)], pick_recv.at[k, xr, pair(p)], pick_sem, (k, xr, p), near
        )

    def swap_copy(k, p):
        at = pl.ds(pl.multiple_of(dat * cap_dev, cap_dev), cap_dev)
        return copy_to(
            swap_send.at[k, pair(p)], rows.at[k * PAIR + x, pair(p), at], swap_sem, (k, p), x_peer
        )

    def swap_arrival(k, p):
        return copy_to(
            swap_send.at[k, pair(p)], own_rows(k, 1, p, dat), swap_sem, (k, p), x_peer
        )

    def y_copy(k, rel, p, of_dat):
        ref = own_rows(k, rel, p, of_dat)
        return copy_to(ref, ref, y_sem, (k, rel, p), y_peer)

    def c_copy(k, rel, p, of_dat):
        ref = own_rows(k, rel, p, of_dat)
        return copy_to(ref, ref, c_sem, (k, rel, p), c_peer)

    def relay_copy(k, rel, p, of_dat):
        ref = own_rows(k, rel, p, of_dat)
        return copy_to(ref, ref, cr_sem, (k, rel, p), c_peer)

    dat_y = dat + PAIR - 2 * PAIR * y
    dat_c = dat + 1 - 2 * c
    dat_yc = dat_y + 1 - 2 * c

    def by_part(value):
        size = pair_e * cap_dev
        return [
            value[p * size : (p + 1) * size].reshape(pair_e, cap_dev, LANES) for p in range(PARTS)
        ]

    def stage_pick(k):
        @pl.when(is_inner)
        def _():
            for xr in range(PAIR):
                near_copy(k, xr).wait_recv()
                for j in range(2):
                    far_copy(k, j, xr).wait_recv()
            found = blocks[k].reshape(LINE * both, LANES)
            for xr in (1, 0):
                at = slice(xr * slots, (xr + 1) * slots)
                got = jnp.dot(pick_far[at, :], found[both:], preferred_element_type=f32)
                got = by_part(got.astype(bf16))
                for p in range(PARTS):
                    pick_send[k, xr, pair(p)] = got[p]
                    pick_copy(k, xr, p).start()
            got = jnp.dot(pick_own[slots:, :], found, preferred_element_type=f32)
            got = by_part(got.astype(bf16))
            for p in range(PARTS):
                swap_send[k, pair(p)] = got[p]
                swap_copy(k, p).start()
            got = jnp.dot(pick_own[:slots, :], found, preferred_element_type=f32)
            got = by_part(got.astype(bf16))
            for p in range(PARTS):
                own_rows(k, 0, p, dat)[...] = got[p]
                y_copy(k, 0, p, dat).start()
                c_copy(k, 0, p, dat).start()

        @pl.when(is_end)
        def _():
            found = blocks[k, 0].reshape(both, LANES)
            got = jnp.dot(pick_own[slots:, :both], found, preferred_element_type=f32)
            got = by_part(got)
            for p in range(PARTS):
                pick_copy(k, 1, p).wait_recv()
                swap_send[k, pair(p)] = (got[p] + pick_recv[k, 1, pair(p)].astype(f32)).astype(bf16)
                swap_copy(k, p).start()
            got = jnp.dot(pick_own[:slots, :both], found, preferred_element_type=f32)
            got = by_part(got)
            for p in range(PARTS):
                pick_copy(k, 0, p).wait_recv()
                own_rows(k, 0, p, dat)[...] = (
                    got[p] + pick_recv[k, 0, pair(p)].astype(f32)
                ).astype(bf16)
                y_copy(k, 0, p, dat).start()
                c_copy(k, 0, p, dat).start()

        for p in range(PARTS):
            for xr in range(PAIR):
                sent.append((pick_copy(k, xr, p), is_inner))
            sent.append((swap_copy(k, p), None))
            sent.append((y_copy(k, 0, p, dat), None))
            sent.append((c_copy(k, 0, p, dat), None))

    def stage_swap(k):
        for p in range(PARTS):
            swap_arrival(k, p).wait_recv()
            send(y_copy(k, 1, p, dat))
            send(c_copy(k, 1, p, dat))

    def stage_relay(k):
        for rel in range(PAIR):
            for p in range(PARTS):
                y_copy(k, rel, p, dat_y).wait_recv()
                send(relay_copy(k, rel, p, dat_y))

    def stage_first(k, p):
        for rel in range(PAIR):
            c_copy(k, rel, p, dat_c).wait_recv()
            relay_copy(k, rel, p, dat_yc).wait_recv()

        for e in range(p * pair_e, (p + 1) * pair_e):
            if k == 0:
                loads[e].wait()
            left = jnp.concatenate([rows[PAIR * k, e], rows[PAIR * k + 1, e]], axis=1)
            total = jnp.dot(left, inner_v[e, k * wide : (k + 1) * wide, :], preferred_element_type=f32)
            if k > 0:
                total += sums[e]
            if k + 1 < chunks:
                sums[e] = total
            else:
                hidden[e] = jnp.maximum(total, 0.0).astype(bf16)

    def core_copy(k, p):
        return copy_to(
            parts.at[k, :, 1 - c, pair(p)], core_recv.at[k, :, pair(p)], rc_sem, (k, p), c_peer
        )

    def back_y(k, p):
        return copy_to(y_send.at[k, pair(p)], y_recv.at[k, pair(p)], ry_sem, (k, p), y_peer)

    def back_x(k, p):
        return copy_to(give.at[k, pair(p)], slots_v.at[k, 1, pair(p)], rx_sem, (k, p), x_peer)

    def raw_copy(k, xr, p):
        return copy_to(
            slots_v.at[k, xr, pair(p)], raw.at[k, xr, pair(p)], raw_sem, (k, xr, p), near
        )

    def dest_copy(k, j, xr, peer):
        return copy_to(
            dest_send.at[k, j, xr], dest_recv.at[k, j, xr], dest_sem, (k, j, xr), peer
        )

    def last_copy(k):
        return copy_to(last_send.at[k], last_recv.at[k], last_sem, (k,), x_peer)

    def stage_second(k, p):
        for e in range(p * pair_e, (p + 1) * pair_e):
            if k == 0:
                loads[experts_dev + e].wait()
            part = jnp.dot(
                hidden[e], outer_v[e, :, k * wide : (k + 1) * wide], preferred_element_type=f32
            ).astype(bf16)
            for d in range(PAIR * PAIR):
                parts[k, d // PAIR, d % PAIR, e] = part[d * cap_dev : (d + 1) * cap_dev]
        send(core_copy(k, p))

    def stage_core(k, p):
        core_copy(k, p).wait_recv()
        theirs = parts[k, 1 - y, c, pair(p)].astype(f32) + core_recv[k, 1 - y, pair(p)].astype(f32)
        y_send[k, pair(p)] = theirs.astype(bf16)
        send(back_y(k, p))
        ours = parts[k, y, c, pair(p)].astype(f32) + core_recv[k, y, pair(p)].astype(f32)
        kept[k, pair(p)] = ours

    def gates():
        at = pl.ds(pl.multiple_of(dat * cap_dev, cap_dev), cap_dev)
        for e in range(experts_dev):
            score = jnp.zeros((cap_dev, LANES), f32)
            for b in range(PAIR * chunks):
                weight = router_ref[e : e + 1, b * LANES : (b + 1) * LANES].astype(f32)
                score += rows[b, e, at].astype(f32) * weight
            gate[e] = jax.nn.sigmoid(jnp.sum(score, axis=-1, keepdims=True))

    def stage_weigh(k, p):
        back_y(k, p).wait_recv()
        summed = kept[k, pair(p)] + y_recv[k, pair(p)].astype(f32)
        own, other = split(gate[pair(p)] * summed)
        give[k, pair(p)] = other.astype(bf16)
        send(back_x(k, p))
        slots_v[k, 0, pair(p)] = own.astype(bf16)
        send(raw_copy(k, 0, p), is_end)

    def stage_cross(k, p):
        back_x(k, p).wait_recv()
        send(raw_copy(k, 1, p), is_end)

    def dest_out(k, j, total, peer):
        for xr in (1, 0):
            dest_send[k, j, xr] = total[xr * tok_rows : (xr + 1) * tok_rows].astype(bf16)
            dest_copy(k, j, xr, peer).start()

    def stage_place(k):
        held = slots_v[k].reshape(PAIR * slots, LANES)

        @pl.when(is_inner)
        def _():
            dest_out(k, 0, jnp.dot(place_own[:both, :], held, preferred_element_type=f32), near)

        at = pl.ds(pl.multiple_of(spot * both, both), both)
        dense[k] = jnp.dot(place_own[at, :], held, preferred_element_type=f32)

    def stage_far(k):
        @pl.when(is_inner)
        def _():
            held = slots_v[k].reshape(PAIR * slots, LANES)
            mine = jnp.dot(place_own[2 * both :, :], held, preferred_element_type=f32)
            for xr in range(PAIR):
                for p in range(PARTS):
                    raw_copy(k, xr, p).wait_recv()
            ends = raw[k].reshape(PAIR * slots, LANES)
            mine += jnp.dot(place_far[both:, :], ends, preferred_element_type=f32)
            dest_out(k, 2, mine[both:], far_end)
            dest_out(k, 1, mine[:both], far_inner)
            dense[k] += jnp.dot(place_far[:both, :], ends, preferred_element_type=f32)

    def stage_total(k):
        for xr in range(PAIR):
            for j, peer in enumerate((near, far_inner, far_end)):
                sent.append((dest_copy(k, j, xr, peer), is_inner))

        def arrived(xr, j):
            dest_copy(k, j, xr, near).wait_recv()
            return dest_recv[k, j, xr].astype(f32)

        def finish(total, xr):
            if xr == 1:
                last_send[k] = total.astype(bf16)
                last_copy(k).start()
            else:
                last_own[k] = total

        @pl.when(is_end)
        def _():
            for xr in (1, 0):
                held = dense[k, xr * tok_rows : (xr + 1) * tok_rows]
                finish(held + arrived(xr, 0) + arrived(xr, 2), xr)

        @pl.when(is_inner)
        def _():
            for xr in (1, 0):
                held = dense[k, xr * tok_rows : (xr + 1) * tok_rows]
                finish(held + arrived(xr, 1), xr)

        sent.append((last_copy(k), None))

    def stage_last(k):
        last_copy(k).wait_recv()
        own, other = last_own[k], last_recv[k].astype(f32)
        cols = slice(k * wide, (k + 1) * wide)
        total = jnp.concatenate([jnp.where(x == 0, own, other), jnp.where(x == 0, other, own)], axis=1)
        out_ref[:, cols] = (tokens_ref[:, cols].astype(f32) + total).astype(bf16)

    for t in range(chunks + 3):
        if t < chunks:
            stage_pick(t)
        if 0 <= t - 1 < chunks:
            stage_swap(t - 1)
        if 0 <= t - 2 < chunks:
            stage_relay(t - 2)
        if 0 <= t - 3 < chunks:
            for p in range(PARTS):
                stage_first(t - 3, p)
                if t - 3 == chunks - 1:
                    stage_second(0, p)

    pieces = [(k, p) for k in range(chunks) for p in range(PARTS)]
    for i in range(PARTS, len(pieces)):
        stage_second(*pieces[i])
        stage_core(*pieces[i - PARTS])
    gates()
    for i in range(len(pieces) - PARTS, len(pieces)):
        stage_core(*pieces[i])

    for t in range(chunks + 4):
        if 0 <= t - 1 < chunks:
            stage_cross(t - 1, 0)
        if t < chunks:
            stage_weigh(t, 0)
        if 0 <= t - 2 < chunks:
            stage_far(t - 2)
        if 0 <= t - 1 < chunks:
            stage_cross(t - 1, 1)
            stage_place(t - 1)
        if t < chunks:
            stage_weigh(t, 1)
        if 0 <= t - 3 < chunks:
            stage_total(t - 3)
        if 0 <= t - 4 < chunks:
            stage_last(t - 4)

    for copy, cond in sent:
        if cond is None:
            copy.wait_send()
        else:
            pl.when(cond)(copy.wait_send)


def kernel_body(tokens, norm_gain, router_weight, inner_weight, outer_weight, slot_tokens, slot_ids):
    del slot_ids
    tok_rows, width = tokens.shape
    experts_dev, cap_dev = slot_tokens.shape
    units = inner_weight.shape[2]
    dat_count = lax.axis_size("dat")
    slots = experts_dev * cap_dev
    wide = PAIR * LANES
    chunks = width // wide
    both = PAIR * tok_rows
    bf16, f32 = jnp.bfloat16, jnp.float32
    vmem = pl.BlockSpec(memory_space=pltpu.VMEM)
    hbm = pl.BlockSpec(memory_space=pl.ANY)
    dma = pltpu.SemaphoreType.DMA

    def buffer(*shape, kind=bf16):
        return pltpu.VMEM(shape, kind)

    return pl.pallas_call(
        moe_kernel,
        out_shape=jax.ShapeDtypeStruct((tok_rows, width), bf16),
        in_specs=[vmem, vmem, vmem, vmem, hbm, hbm],
        out_specs=vmem,
        scratch_shapes=[
            buffer(experts_dev, width, units),
            buffer(experts_dev, units, width),
            buffer(LINE, experts_dev, cap_dev, kind=jnp.int32),
            buffer(PAIR * slots, LINE * both),
            buffer(LINE * both, PAIR * slots),
            buffer(PAIR * slots, (LINE - 1) * both),
            buffer((LINE - 1) * both, PAIR * slots),
            buffer(chunks, LINE, PAIR, tok_rows, LANES),
            buffer(chunks, tok_rows, LANES),
            buffer(chunks, PAIR, experts_dev, cap_dev, LANES),
            buffer(chunks, PAIR, experts_dev, cap_dev, LANES),
            buffer(chunks, experts_dev, cap_dev, LANES),
            buffer(PAIR * chunks, experts_dev, dat_count * cap_dev, LANES),
            buffer(experts_dev, dat_count * cap_dev, units, kind=f32),
            buffer(experts_dev, dat_count * cap_dev, units),
            buffer(experts_dev, cap_dev, 1, kind=f32),
            buffer(chunks, PAIR, PAIR, experts_dev, cap_dev, wide),
            buffer(chunks, PAIR, experts_dev, cap_dev, wide),
            buffer(chunks, experts_dev, cap_dev, wide),
            buffer(chunks, experts_dev, cap_dev, wide),
            buffer(chunks, experts_dev, cap_dev, wide, kind=f32),
            buffer(chunks, experts_dev, cap_dev, LANES),
            buffer(chunks, PAIR, experts_dev, cap_dev, LANES),
            buffer(chunks, PAIR, experts_dev, cap_dev, LANES),
            buffer(chunks, both, LANES, kind=f32),
            buffer(chunks, LINE - 1, PAIR, tok_rows, LANES),
            buffer(chunks, LINE - 1, PAIR, tok_rows, LANES),
            buffer(chunks, tok_rows, LANES),
            buffer(chunks, tok_rows, LANES),
            buffer(chunks, tok_rows, LANES, kind=f32),
            dma((2, experts_dev)),
            dma((2, 3)),
            dma((2, chunks)),
            dma((2, chunks, PAIR)),
            dma((2, chunks, 2, PAIR)),
            dma((2, chunks, PAIR, PARTS)),
            dma((2, chunks, PARTS)),
            dma((2, chunks, PAIR, PARTS)),
            dma((2, chunks, PAIR, PARTS)),
            dma((2, chunks, PAIR, PARTS)),
            dma((2, chunks, PARTS)),
            dma((2, chunks, PARTS)),
            dma((2, chunks, PARTS)),
            dma((2, chunks, PAIR, PARTS)),
            dma((2, chunks, LINE - 1, PAIR)),
            dma((2, chunks)),
        ],
        compiler_params=pltpu.CompilerParams(
            collective_id=0, has_side_effects=True, vmem_limit_bytes=60 * 1024 * 1024
        ),
    )(tokens, norm_gain.reshape(1, width), router_weight.T, slot_tokens, inner_weight, outer_weight)


def solution(mesh):
    fits = mesh.shape["dat"] == PAIR * PAIR and mesh.shape["exp"] == PAIR * LINE
    chosen = kernel_body if fits else body
    in_specs = (
        P(("exp", "dat"), None),
        P(),
        P(None, "exp"),
        P("exp", None, "dat"),
        P("exp", "dat", None),
        P("exp", "dat"),
        P(("exp", "dat"), None),
    )
    out_specs = P(("exp", "dat"), None)
    return jax.shard_map(chosen, mesh=mesh, in_specs=in_specs, out_specs=out_specs, check_vma=False)
```

```python
import jax
import jax.numpy as jnp
from jax import lax
from jax.experimental import pallas as pl
from jax.experimental.pallas import tpu as pltpu
from jax.sharding import PartitionSpec as P

EPSILON = 1e-06


def normalize(tokens, norm_gain):
    values = tokens.astype(jnp.float32)
    scale = lax.rsqrt(jnp.mean(values * values, axis=-1, keepdims=True) + EPSILON)
    return (values * scale * norm_gain).astype(jnp.bfloat16)


def owner_places(slot_ids, experts_dev, capacity, bucket):
    flat_ids = slot_ids.reshape(-1)
    source = flat_ids // capacity // experts_dev
    before = (source[:, None] == source[None, :]) & (flat_ids[None, :] < flat_ids[:, None])
    ranks_in = jnp.sum(before.astype(jnp.int32), axis=1)
    return (source * bucket + ranks_in).reshape(slot_ids.shape)


def expert_places(token_ids, slot_keys, tok_rows, dat_count, bucket):
    owner_of = token_ids // (tok_rows * dat_count)
    before = (owner_of[:, None] == owner_of[None, :]) & (slot_keys[None, :] < slot_keys[:, None])
    ranks_in = jnp.sum(before.astype(jnp.int32), axis=1)
    return owner_of * bucket + ranks_in


def body(tokens, norm_gain, router_weight, inner_weight, outer_weight, slot_tokens, slot_ids):
    exp_count = lax.axis_size("exp")
    dat_count = lax.axis_size("dat")
    tok_rows, width = tokens.shape
    experts_dev, cap_dev = slot_tokens.shape
    bucket = 6 * tok_rows // exp_count
    normed = normalize(tokens, norm_gain)
    picked = slot_tokens.T.reshape(-1)
    expert_iota = lax.broadcasted_iota(jnp.int32, (cap_dev, experts_dev), 1)
    column_iota = lax.broadcasted_iota(jnp.int32, (cap_dev, experts_dev), 0)
    slot_keys = (expert_iota * cap_dev + column_iota).reshape(-1)
    senders = expert_places(picked, slot_keys, tok_rows, dat_count, bucket)
    receivers = owner_places(slot_ids, experts_dev, cap_dev * dat_count, bucket)
    lookup = jnp.any(
        lax.broadcasted_iota(jnp.int32, (exp_count * bucket, 1, 1), 0) == receivers[None], axis=2
    )
    outgoing = jnp.dot(lookup.astype(jnp.bfloat16), normed, preferred_element_type=jnp.float32)
    outgoing = outgoing.astype(jnp.bfloat16).reshape(exp_count, bucket, width)
    arrived = lax.all_to_all(outgoing, "exp", split_axis=0, concat_axis=0, tiled=True).reshape(
        exp_count * bucket, width
    )
    gathered_rows = jnp.take(arrived, senders, axis=0)
    gathered_rows = gathered_rows.reshape(cap_dev, experts_dev, width)
    gate_score = jax.nn.sigmoid(
        jnp.einsum("ced,de->ce", gathered_rows, router_weight, preferred_element_type=jnp.float32)
    )
    inner = jnp.einsum(
        "ced,edf->cef",
        lax.all_gather(gathered_rows, "dat", axis=0, tiled=True),
        inner_weight,
        preferred_element_type=jnp.float32,
    )
    hidden = jax.nn.relu(inner).astype(jnp.bfloat16)
    expert_out = lax.psum_scatter(
        jnp.einsum("cef,efd->ced", hidden, outer_weight, preferred_element_type=jnp.float32).astype(
            jnp.bfloat16
        ),
        "dat",
        scatter_dimension=0,
        tiled=True,
    ).astype(jnp.float32)
    weighted = (gate_score[:, :, None] * expert_out).astype(jnp.bfloat16).reshape(-1, width)
    placing = lax.broadcasted_iota(jnp.int32, (exp_count * bucket, 1), 0) == senders[None, :]
    returning = jnp.dot(placing.astype(jnp.bfloat16), weighted, preferred_element_type=jnp.float32)
    returning = returning.astype(jnp.bfloat16).reshape(exp_count, bucket, width)
    came_back = lax.all_to_all(returning, "exp", split_axis=0, concat_axis=0, tiled=True).reshape(
        exp_count * bucket, width
    )
    combine_table = jnp.sum(
        (
            lax.broadcasted_iota(jnp.int32, (1, 1, exp_count * bucket), 2) == receivers[:, :, None]
        ).astype(jnp.float32),
        axis=1,
    )
    combined = jnp.dot(
        combine_table.astype(jnp.bfloat16), came_back, preferred_element_type=jnp.float32
    )
    return (tokens.astype(jnp.float32) + combined).astype(jnp.bfloat16)


MESH = pl.DeviceIdType.MESH
PAIR = 2
LINE = 4
LANES = 128
PARTS = 2


def moe_kernel(
    tokens_hbm, gain_hbm, router_hbm, ids_hbm, inner_hbm, outer_hbm, out_ref,
    tokens_ref, gain_ref, router_ref, ids_ref, inner_v, outer_v, ids_all, pick_own, place_own, pick_far, place_far,
    blocks, cross, pick_send, pick_recv, swap_send, rows, sums, hidden, gate,
    parts, core_recv, y_send, y_recv, kept, give, slots_v, raw, dense, dest_send, dest_recv,
    last_send, last_recv, last_own,
    w_sem, out_sem, ids_sem, x_sem, near_sem, far_sem, pick_sem, swap_sem, y_sem, c_sem, cr_sem,
    rc_sem, ry_sem, rx_sem, raw_sem, dest_sem, last_sem,
):
    chunks = blocks.shape[0]
    tok_rows = tokens_ref.shape[0]
    experts_dev, cap_dev = ids_ref.shape
    slots = experts_dev * cap_dev
    both = PAIR * tok_rows
    wide = PAIR * LANES
    pair_e = experts_dev // PARTS
    bf16, f32 = jnp.bfloat16, jnp.float32
    exp = lax.axis_index("exp")
    dat = lax.axis_index("dat")
    dat_count = lax.axis_size("dat")
    z, x = exp // PAIR, exp % PAIR
    y, c = dat // PAIR, dat % PAIR
    half = z // PAIR
    spot = z + half * (LINE - 1 - 2 * z)
    is_end = spot == 0
    is_inner = spot == 1

    def line_z(q):
        return q + half * (LINE - 1 - 2 * q)

    near = (line_z(1 - spot) * PAIR + x, dat)
    far_inner = (line_z(2) * PAIR + x, dat)
    far_end = (line_z(3) * PAIR + x, dat)
    x_peer = (exp + 1 - 2 * x, dat)
    y_peer = (exp, dat + PAIR - 2 * PAIR * y)
    c_peer = (exp, dat + 1 - 2 * c)
    diag = (line_z(1 - spot) * PAIR + 1 - x, dat)

    def copy_to(src, dst, stage, sems, where, peer):
        return pltpu.make_async_remote_copy(
            src_ref=src, dst_ref=dst, send_sem=out_sem.at[stage],
            recv_sem=sems.at[where], device_id=peer, device_id_type=MESH,
        )

    def send(copy, cond=None):
        if cond is None:
            copy.start()
        else:
            pl.when(cond)(copy.start)

    loads = []
    for e in range(experts_dev):
        loads.append(pltpu.make_async_copy(inner_hbm.at[e], inner_v.at[e], w_sem.at[0]))
    for e in range(experts_dev):
        loads.append(pltpu.make_async_copy(outer_hbm.at[e], outer_v.at[e], w_sem.at[1]))
    inner_load = pltpu.make_async_copy(inner_hbm, inner_v, w_sem.at[0])
    outer_load = pltpu.make_async_copy(outer_hbm, outer_v, w_sem.at[1])

    barrier = pltpu.get_barrier_semaphore()
    for peer in (near, diag, far_inner, x_peer, y_peer, c_peer):
        pl.semaphore_signal(barrier, inc=1, device_id=peer, device_id_type=MESH)

    @pl.when(is_inner)
    def _():
        pl.semaphore_signal(barrier, inc=1, device_id=far_end, device_id_type=MESH)

    smalls = []
    for i, (src, dst) in enumerate(
        ((ids_hbm, ids_ref), (tokens_hbm, tokens_ref), (gain_hbm, gain_ref), (router_hbm, router_ref))
    ):
        smalls.append(pltpu.make_async_copy(src, dst, w_sem.at[2 + i]))
        smalls[i].start()
    for load in loads:
        load.start()
    smalls[1].wait()
    smalls[2].wait()

    values = tokens_ref[...].astype(f32)
    scale = lax.rsqrt(jnp.mean(values * values, axis=-1, keepdims=True) + EPSILON)
    normed = values * scale * gain_ref[...]

    def split(value):
        low, high = value[..., :LANES], value[..., LANES:]
        return jnp.where(x == 0, low, high), jnp.where(x == 0, high, low)

    for k in range(chunks):
        own, other = split(normed[:, k * wide : (k + 1) * wide])
        blocks[k, spot, 0] = own.astype(bf16)
        cross[k] = other.astype(bf16)

    def one_hots(ids, side, pick, place, first):
        row = jnp.concatenate([ids[e : e + 1, :] for e in range(experts_dev)], axis=1)
        column = jnp.broadcast_to(row, (LANES, slots)).T
        lane = lax.broadcasted_iota(jnp.int32, (slots, tok_rows), 1)
        line = lax.broadcasted_iota(jnp.int32, (tok_rows, slots), 0)
        at = slice(side * slots, (side + 1) * slots)
        for q in range(first, LINE):
            for xr in range(PAIR):
                x_of = x if xr == 0 else 1 - x
                base = ((line_z(q) * PAIR + x_of) * dat_count + dat) * tok_rows
                start = ((q - first) * PAIR + xr) * tok_rows
                span = slice(start, start + tok_rows)
                pick[at, span] = (column == lane + base).astype(f32).astype(bf16)
                place[span, at] = (row == line + base).astype(f32).astype(bf16)

    smalls[0].wait()
    one_hots(ids_ref, 0, pick_own, place_own, 0)

    pl.semaphore_wait(barrier, 6 + is_inner.astype(jnp.int32))

    def cross_copy(k):
        return copy_to(cross.at[k], blocks.at[k, spot, 1], 0, x_sem, (k,), x_peer)

    ids_x = copy_to(ids_ref, ids_all.at[1], 1, ids_sem, (0,), x_peer)
    ids_near = copy_to(ids_ref, ids_all.at[2], 2, ids_sem, (1,), near)
    ids_diag = copy_to(ids_ref, ids_all.at[3], 2, ids_sem, (1,), diag)
    ids_both = copy_to(ids_all.at[2:4], ids_all.at[2:4], 2, ids_sem, (1,), near)

    def near_copy(k, xr):
        ref = blocks.at[k, 0, xr]
        return copy_to(ref, ref, 3, near_sem, (k,), near)

    def far_copy(k, xr):
        return copy_to(blocks.at[k, spot, xr], blocks.at[k, 3 - spot, xr], 4, far_sem, (k,), far_inner)

    def block_send(k, xr):
        send(far_copy(k, xr))
        send(near_copy(k, xr), is_end)

    send(cross_copy(0))
    block_send(0, 0)
    send(ids_x)
    send(ids_near, is_end)
    send(ids_diag, is_end)
    send(cross_copy(1))
    block_send(1, 0)
    for k in range(2, chunks):
        send(cross_copy(k))
    for k in range(chunks):
        cross_copy(k).wait_recv()
        block_send(k, 1)
        if k + 2 < chunks:
            block_send(k + 2, 0)
    ids_x.wait_recv()
    one_hots(ids_all.at[1], 1, pick_own, place_own, 0)

    @pl.when(is_inner)
    def _():
        ids_both.wait_recv()
        one_hots(ids_all.at[2], 0, pick_far, place_far, 1)
        one_hots(ids_all.at[3], 1, pick_far, place_far, 1)

    def pair(p):
        return slice(p * pair_e, (p + 1) * pair_e)

    def own_rows(k, rel, p, of_dat):
        feature = k * PAIR + (x if rel == 0 else 1 - x)
        at = pl.ds(pl.multiple_of(of_dat * cap_dev, cap_dev), cap_dev)
        return rows.at[feature, pair(p), at]

    def dat_at(of_dat):
        return pl.ds(pl.multiple_of(of_dat * cap_dev, cap_dev), cap_dev)

    def pick_copy(k, xr, p):
        return copy_to(
            pick_send.at[k, xr, pair(p)], pick_recv.at[k, xr, pair(p)], 5, pick_sem, (k, xr, p), near
        )

    def swap_copy(k, p):
        return copy_to(
            swap_send.at[k, pair(p)], own_rows(k, 0, p, dat), 6, swap_sem, (k, p), x_peer
        )

    def y_copy(k, rel, p, of_dat):
        ref = own_rows(k, rel, p, of_dat)
        return copy_to(ref, ref, 7, y_sem, (k, rel, p), y_peer)

    def c_copy(k, rel, p, of_dat):
        ref = own_rows(k, rel, p, of_dat)
        return copy_to(ref, ref, 8, c_sem, (k, p), c_peer)

    def relay_copy(k, rel, p, of_dat):
        ref = own_rows(k, rel, p, of_dat)
        return copy_to(ref, ref, 9, cr_sem, (k, p), c_peer)

    def both_rows(k, p, of_dat):
        return rows.at[k * PAIR : (k + 1) * PAIR, pair(p), dat_at(of_dat)]

    dat_y = dat + PAIR - 2 * PAIR * y
    dat_c = dat + 1 - 2 * c
    dat_yc = dat_y + 1 - 2 * c

    def by_part(value):
        size = pair_e * cap_dev
        return [
            value[p * size : (p + 1) * size].reshape(pair_e, cap_dev, LANES) for p in range(PARTS)
        ]

    def sides(k):
        return (1, 0) if k + 1 == chunks else (0, 1)

    def stage_far_pick(k):
        @pl.when(is_inner)
        def _():
            near_all, far_all = blocks.at[k, 0], blocks.at[k, 2:4]
            copy_to(near_all, near_all, 3, near_sem, (k,), near).wait_recv()
            copy_to(far_all, far_all, 4, far_sem, (k,), far_inner).wait_recv()
            found = blocks[k].reshape(LINE * both, LANES)
            for xr in sides(k):
                at = slice(xr * slots, (xr + 1) * slots)
                got = jnp.dot(pick_far[at, :], found[both:], preferred_element_type=f32)
                got = by_part(got.astype(bf16))
                for p in range(PARTS):
                    pick_send[k, xr, pair(p)] = got[p]
                    pick_copy(k, xr, p).start()

    def hand_on(k, xr, p, value):
        if xr == 1:
            swap_send[k, pair(p)] = value
            swap_copy(k, p).start()
        else:
            own_rows(k, 0, p, dat)[...] = value
            y_copy(k, 0, p, dat).start()
            c_copy(k, 0, p, dat).start()

    def stage_pick(k):
        @pl.when(is_inner)
        def _():
            found = blocks[k].reshape(LINE * both, LANES)
            for xr in (1, 0):
                at = slice(xr * slots, (xr + 1) * slots)
                got = jnp.dot(pick_own[at, :], found, preferred_element_type=f32)
                got = by_part(got.astype(bf16))
                for p in range(PARTS):
                    hand_on(k, xr, p, got[p])

        @pl.when(is_end)
        def _():
            found = blocks[k, 0].reshape(both, LANES)
            for xr in sides(k):
                at = slice(xr * slots, (xr + 1) * slots)
                got = by_part(jnp.dot(pick_own[at, :both], found, preferred_element_type=f32))
                for p in range(PARTS):
                    pick_copy(k, xr, p).wait_recv()
                    here = got[p] + pick_recv[k, xr, pair(p)].astype(f32)
                    hand_on(k, xr, p, here.astype(bf16))

    def stage_swap(k):
        for p in range(PARTS):
            ref = own_rows(k, 1, p, dat)
            copy_to(ref, ref, 6, swap_sem, (k, p), x_peer).wait_recv()
            send(y_copy(k, 1, p, dat))
            send(c_copy(k, 1, p, dat))

    def stage_relay(k, rel):
        for p in range(PARTS):
            y_copy(k, rel, p, dat_y).wait_recv()
            send(relay_copy(k, rel, p, dat_y))

    def stage_first(k, p):
        for sems, stage, of_dat in ((c_sem, 8, dat_c), (cr_sem, 9, dat_yc)):
            ref = both_rows(k, p, of_dat)
            copy_to(ref, ref, stage, sems, (k, p), c_peer).wait_recv()
        if k == 0 and p == 0:
            inner_load.wait()

        for e in range(p * pair_e, (p + 1) * pair_e):
            left = jnp.concatenate([rows[PAIR * k, e], rows[PAIR * k + 1, e]], axis=1)
            total = jnp.dot(left, inner_v[e, k * wide : (k + 1) * wide, :], preferred_element_type=f32)
            if k > 0:
                total += sums[e]
            if k + 1 < chunks:
                sums[e] = total
            else:
                hidden[e] = jnp.maximum(total, 0.0).astype(bf16)

    def core_copy(k, p):
        return copy_to(
            parts.at[k, :, 1 - c, pair(p)], core_recv.at[k, :, pair(p)], 10, rc_sem, (k, p), c_peer
        )

    def back_y(k, p):
        return copy_to(y_send.at[k, pair(p)], y_recv.at[k, pair(p)], 11, ry_sem, (k, p), y_peer)

    def back_x(k, p):
        return copy_to(give.at[k, pair(p)], slots_v.at[k, 1, pair(p)], 12, rx_sem, (k, p), x_peer)

    def raw_copy(k, xr, p):
        return copy_to(
            slots_v.at[k, xr, pair(p)], raw.at[k, xr, pair(p)], 13, raw_sem, (k,), near
        )

    def dest_copy(k, j, xr, peer):
        return copy_to(
            dest_send.at[k, j, xr], dest_recv.at[k, min(j, 1), xr], 14, dest_sem, (k, xr), peer
        )

    def last_copy(k):
        return copy_to(last_send.at[k], last_recv.at[k], 15, last_sem, (k,), x_peer)

    def stage_second(k, p):
        if k == 0 and p == 0:
            outer_load.wait()
        for e in range(p * pair_e, (p + 1) * pair_e):
            part = jnp.dot(
                hidden[e], outer_v[e, :, k * wide : (k + 1) * wide], preferred_element_type=f32
            ).astype(bf16)
            for d in range(PAIR * PAIR):
                parts[k, d // PAIR, d % PAIR, e] = part[d * cap_dev : (d + 1) * cap_dev]
        send(core_copy(k, p))

    def stage_core(k, p):
        core_copy(k, p).wait_recv()
        theirs = parts[k, 1 - y, c, pair(p)].astype(f32) + core_recv[k, 1 - y, pair(p)].astype(f32)
        y_send[k, pair(p)] = theirs.astype(bf16)
        send(back_y(k, p))
        ours = parts[k, y, c, pair(p)].astype(f32) + core_recv[k, y, pair(p)].astype(f32)
        kept[k, pair(p)] = ours

    def gates():
        smalls[3].wait()
        at = pl.ds(pl.multiple_of(dat * cap_dev, cap_dev), cap_dev)
        for e in range(experts_dev):
            score = jnp.zeros((cap_dev, LANES), f32)
            for b in range(PAIR * chunks):
                weight = router_ref[e : e + 1, b * LANES : (b + 1) * LANES].astype(f32)
                score += rows[b, e, at].astype(f32) * weight
            gate[e] = jax.nn.sigmoid(jnp.sum(score, axis=-1, keepdims=True))

    def stage_weigh(k, p):
        back_y(k, p).wait_recv()
        summed = kept[k, pair(p)] + y_recv[k, pair(p)].astype(f32)
        own, other = split(gate[pair(p)] * summed)
        give[k, pair(p)] = other.astype(bf16)
        send(back_x(k, p))
        slots_v[k, 0, pair(p)] = own.astype(bf16)
        send(raw_copy(k, 0, p), is_end)

    def stage_cross(k, p):
        back_x(k, p).wait_recv()
        send(raw_copy(k, 1, p), is_end)

    def dest_out(k, j, total, peer):
        for xr in (1, 0):
            dest_send[k, j, xr] = total[xr * tok_rows : (xr + 1) * tok_rows].astype(bf16)
            dest_copy(k, j, xr, peer).start()

    def stage_place(k):
        held = slots_v[k].reshape(PAIR * slots, LANES)

        @pl.when(is_inner)
        def _():
            dest_out(k, 0, jnp.dot(place_own[:both, :], held, preferred_element_type=f32), near)

        at = pl.ds(pl.multiple_of(spot * both, both), both)
        dense[k] = jnp.dot(place_own[at, :], held, preferred_element_type=f32)

    def stage_far(k):
        @pl.when(is_inner)
        def _():
            held = slots_v[k].reshape(PAIR * slots, LANES)
            mine = jnp.dot(place_own[2 * both :, :], held, preferred_element_type=f32)
            copy_to(raw.at[k], raw.at[k], 13, raw_sem, (k,), near).wait_recv()
            ends = raw[k].reshape(PAIR * slots, LANES)
            mine += jnp.dot(place_far[both:, :], ends, preferred_element_type=f32)
            dest_out(k, 2, mine[both:], far_end)
            dest_out(k, 1, mine[:both], far_inner)
            dense[k] += jnp.dot(place_far[:both, :], ends, preferred_element_type=f32)

    def stage_total(k):
        def finish(total, xr):
            if xr == 1:
                last_send[k] = total.astype(bf16)
                last_copy(k).start()
            else:
                last_own[k] = total

        def arrived(xr, ref):
            copy_to(ref, ref, 14, dest_sem, (k, xr), near).wait_recv()
            return dense[k, xr * tok_rows : (xr + 1) * tok_rows]

        @pl.when(is_end)
        def _():
            for xr in (1, 0):
                held = arrived(xr, dest_recv.at[k, :, xr])
                finish(held + dest_recv[k, 0, xr].astype(f32) + dest_recv[k, 1, xr].astype(f32), xr)

        @pl.when(is_inner)
        def _():
            for xr in (1, 0):
                held = arrived(xr, dest_recv.at[k, 1, xr])
                finish(held + dest_recv[k, 1, xr].astype(f32), xr)

    def stage_last(k):
        last_copy(k).wait_recv()
        own, other = last_own[k], last_recv[k].astype(f32)
        cols = slice(k * wide, (k + 1) * wide)
        total = jnp.concatenate([jnp.where(x == 0, own, other), jnp.where(x == 0, other, own)], axis=1)
        out_ref[:, cols] = (tokens_ref[:, cols].astype(f32) + total).astype(bf16)

    last = chunks - 1

    def run_first(k):
        for p in range(PARTS):
            stage_first(k, p)
            if k == last:
                stage_second(0, p)

    order = []
    for k in range(chunks):
        order += [
            (2.8 * k - 2.65, stage_far_pick, (k,)),
            (2.8 * k, stage_pick, (k,)),
            (2.8 * k + 3.1, stage_swap, (k,)),
            (2.8 * k + 3.9, stage_relay, (k, 0)),
            (2.8 * k + 7.0, stage_relay, (k, 1)),
            (2.8 * k + 8.9, run_first, (k,)),
        ]
    for _, stage, where in sorted(order, key=lambda step: step[0]):
        stage(*where)

    pieces = [(k, p) for k in range(chunks) for p in range(PARTS)]
    for i in range(PARTS, len(pieces)):
        stage_second(*pieces[i])
        stage_core(*pieces[i - PARTS])
    gates()
    for i in range(len(pieces) - PARTS, len(pieces)):
        stage_core(*pieces[i])

    for i in range(len(pieces) + 2):
        if i < len(pieces):
            stage_weigh(*pieces[i])
        if i == len(pieces):
            stage_far(0)
        if i >= 2:
            stage_cross(*pieces[i - 2])
            if i % 2 == 1:
                stage_place(i // 2 - 1)
    for t in range(1, chunks + 3):
        if t < chunks:
            stage_far(t)
        if t >= 3:
            stage_last(t - 3)
        if 1 <= t <= chunks:
            stage_total(t - 1)

    def sent(ref, stage, cond=None):
        done = copy_to(ref, ref, stage, ids_sem, (0,), x_peer)
        if cond is None:
            done.wait_send()
        else:
            pl.when(cond)(done.wait_send)

    own_all = rows.at[:, :, dat_at(dat)]
    sent(cross, 0)
    sent(ids_ref, 1)
    sent(ids_all.at[2:4], 2, is_end)
    sent(blocks.at[0], 3, is_end)
    sent(blocks.at[0], 4)
    sent(pick_send, 5, is_inner)
    sent(swap_send, 6)
    for stage in (7, 8, 9):
        sent(own_all, stage)
    sent(parts.at[:, :, 1 - c], 10)
    sent(y_send, 11)
    sent(give, 12)
    sent(slots_v, 13, is_end)
    sent(dest_send, 14, is_inner)
    sent(last_send, 15)


def kernel_body(tokens, norm_gain, router_weight, inner_weight, outer_weight, slot_tokens, slot_ids):
    del slot_ids
    tok_rows, width = tokens.shape
    experts_dev, cap_dev = slot_tokens.shape
    units = inner_weight.shape[2]
    dat_count = lax.axis_size("dat")
    slots = experts_dev * cap_dev
    wide = PAIR * LANES
    chunks = width // wide
    both = PAIR * tok_rows
    bf16, f32 = jnp.bfloat16, jnp.float32
    vmem = pl.BlockSpec(memory_space=pltpu.VMEM)
    hbm = pl.BlockSpec(memory_space=pltpu.HBM)
    dma = pltpu.SemaphoreType.DMA

    def buffer(*shape, kind=bf16):
        return pltpu.VMEM(shape, kind)

    return pl.pallas_call(
        moe_kernel,
        out_shape=jax.ShapeDtypeStruct((tok_rows, width), bf16),
        in_specs=[hbm] * 6,
        out_specs=vmem,
        scratch_shapes=[
            buffer(tok_rows, width),
            buffer(1, width, kind=f32),
            buffer(experts_dev, width),
            buffer(experts_dev, cap_dev, kind=jnp.int32),
            buffer(experts_dev, width, units),
            buffer(experts_dev, units, width),
            buffer(LINE, experts_dev, cap_dev, kind=jnp.int32),
            buffer(PAIR * slots, LINE * both),
            buffer(LINE * both, PAIR * slots),
            buffer(PAIR * slots, (LINE - 1) * both),
            buffer((LINE - 1) * both, PAIR * slots),
            buffer(chunks, LINE, PAIR, tok_rows, LANES),
            buffer(chunks, tok_rows, LANES),
            buffer(chunks, PAIR, experts_dev, cap_dev, LANES),
            buffer(chunks, PAIR, experts_dev, cap_dev, LANES),
            buffer(chunks, experts_dev, cap_dev, LANES),
            buffer(PAIR * chunks, experts_dev, dat_count * cap_dev, LANES),
            buffer(experts_dev, dat_count * cap_dev, units, kind=f32),
            buffer(experts_dev, dat_count * cap_dev, units),
            buffer(experts_dev, cap_dev, 1, kind=f32),
            buffer(chunks, PAIR, PAIR, experts_dev, cap_dev, wide),
            buffer(chunks, PAIR, experts_dev, cap_dev, wide),
            buffer(chunks, experts_dev, cap_dev, wide),
            buffer(chunks, experts_dev, cap_dev, wide),
            buffer(chunks, experts_dev, cap_dev, wide, kind=f32),
            buffer(chunks, experts_dev, cap_dev, LANES),
            buffer(chunks, PAIR, experts_dev, cap_dev, LANES),
            buffer(chunks, PAIR, experts_dev, cap_dev, LANES),
            buffer(chunks, both, LANES, kind=f32),
            buffer(chunks, LINE - 1, PAIR, tok_rows, LANES),
            buffer(chunks, 2, PAIR, tok_rows, LANES),
            buffer(chunks, tok_rows, LANES),
            buffer(chunks, tok_rows, LANES),
            buffer(chunks, tok_rows, LANES, kind=f32),
            dma((6,)),
            dma((16,)),
            dma((2,)),
            dma((chunks,)),
            dma((chunks,)),
            dma((chunks,)),
            dma((chunks, PAIR, PARTS)),
            dma((chunks, PARTS)),
            dma((chunks, PAIR, PARTS)),
            dma((chunks, PARTS)),
            dma((chunks, PARTS)),
            dma((chunks, PARTS)),
            dma((chunks, PARTS)),
            dma((chunks, PARTS)),
            dma((chunks,)),
            dma((chunks, PAIR)),
            dma((chunks,)),
        ],
        compiler_params=pltpu.CompilerParams(
            collective_id=0, has_side_effects=True, vmem_limit_bytes=48 * 1024 * 1024
        ),
    )(
        *(
            pltpu.with_memory_space_constraint(array, pltpu.HBM)
            for array in (tokens, norm_gain.reshape(1, width), router_weight.T, slot_tokens)
        ),
        inner_weight,
        outer_weight,
    )


def solution(mesh):
    fits = mesh.shape["dat"] == PAIR * PAIR and mesh.shape["exp"] == PAIR * LINE
    chosen = kernel_body if fits else body
    in_specs = (
        P(("exp", "dat"), None),
        P(),
        P(None, "exp"),
        P("exp", None, "dat"),
        P("exp", "dat", None),
        P("exp", "dat"),
        P(("exp", "dat"), None),
    )
    out_specs = P(("exp", "dat"), None)
    return jax.shard_map(chosen, mesh=mesh, in_specs=in_specs, out_specs=out_specs, check_vma=False)
```

```python
import jax
import jax.numpy as jnp
from jax import lax
from jax.experimental import pallas as pl
from jax.experimental.pallas import tpu as pltpu
from jax.sharding import PartitionSpec as P

EPSILON = 1e-06


def normalize(tokens, norm_gain):
    values = tokens.astype(jnp.float32)
    scale = lax.rsqrt(jnp.mean(values * values, axis=-1, keepdims=True) + EPSILON)
    return (values * scale * norm_gain).astype(jnp.bfloat16)


def owner_places(slot_ids, experts_dev, capacity, bucket):
    flat_ids = slot_ids.reshape(-1)
    source = flat_ids // capacity // experts_dev
    before = (source[:, None] == source[None, :]) & (flat_ids[None, :] < flat_ids[:, None])
    ranks_in = jnp.sum(before.astype(jnp.int32), axis=1)
    return (source * bucket + ranks_in).reshape(slot_ids.shape)


def expert_places(token_ids, slot_keys, tok_rows, dat_count, bucket):
    owner_of = token_ids // (tok_rows * dat_count)
    before = (owner_of[:, None] == owner_of[None, :]) & (slot_keys[None, :] < slot_keys[:, None])
    ranks_in = jnp.sum(before.astype(jnp.int32), axis=1)
    return owner_of * bucket + ranks_in


def body(tokens, norm_gain, router_weight, inner_weight, outer_weight, slot_tokens, slot_ids):
    exp_count = lax.axis_size("exp")
    dat_count = lax.axis_size("dat")
    tok_rows, width = tokens.shape
    experts_dev, cap_dev = slot_tokens.shape
    bucket = 6 * tok_rows // exp_count
    normed = normalize(tokens, norm_gain)
    picked = slot_tokens.T.reshape(-1)
    expert_iota = lax.broadcasted_iota(jnp.int32, (cap_dev, experts_dev), 1)
    column_iota = lax.broadcasted_iota(jnp.int32, (cap_dev, experts_dev), 0)
    slot_keys = (expert_iota * cap_dev + column_iota).reshape(-1)
    senders = expert_places(picked, slot_keys, tok_rows, dat_count, bucket)
    receivers = owner_places(slot_ids, experts_dev, cap_dev * dat_count, bucket)
    lookup = jnp.any(
        lax.broadcasted_iota(jnp.int32, (exp_count * bucket, 1, 1), 0) == receivers[None], axis=2
    )
    outgoing = jnp.dot(lookup.astype(jnp.bfloat16), normed, preferred_element_type=jnp.float32)
    outgoing = outgoing.astype(jnp.bfloat16).reshape(exp_count, bucket, width)
    arrived = lax.all_to_all(outgoing, "exp", split_axis=0, concat_axis=0, tiled=True).reshape(
        exp_count * bucket, width
    )
    gathered_rows = jnp.take(arrived, senders, axis=0)
    gathered_rows = gathered_rows.reshape(cap_dev, experts_dev, width)
    gate_score = jax.nn.sigmoid(
        jnp.einsum("ced,de->ce", gathered_rows, router_weight, preferred_element_type=jnp.float32)
    )
    inner = jnp.einsum(
        "ced,edf->cef",
        lax.all_gather(gathered_rows, "dat", axis=0, tiled=True),
        inner_weight,
        preferred_element_type=jnp.float32,
    )
    hidden = jax.nn.relu(inner).astype(jnp.bfloat16)
    expert_out = lax.psum_scatter(
        jnp.einsum("cef,efd->ced", hidden, outer_weight, preferred_element_type=jnp.float32).astype(
            jnp.bfloat16
        ),
        "dat",
        scatter_dimension=0,
        tiled=True,
    ).astype(jnp.float32)
    weighted = (gate_score[:, :, None] * expert_out).astype(jnp.bfloat16).reshape(-1, width)
    placing = lax.broadcasted_iota(jnp.int32, (exp_count * bucket, 1), 0) == senders[None, :]
    returning = jnp.dot(placing.astype(jnp.bfloat16), weighted, preferred_element_type=jnp.float32)
    returning = returning.astype(jnp.bfloat16).reshape(exp_count, bucket, width)
    came_back = lax.all_to_all(returning, "exp", split_axis=0, concat_axis=0, tiled=True).reshape(
        exp_count * bucket, width
    )
    combine_table = jnp.sum(
        (
            lax.broadcasted_iota(jnp.int32, (1, 1, exp_count * bucket), 2) == receivers[:, :, None]
        ).astype(jnp.float32),
        axis=1,
    )
    combined = jnp.dot(
        combine_table.astype(jnp.bfloat16), came_back, preferred_element_type=jnp.float32
    )
    return (tokens.astype(jnp.float32) + combined).astype(jnp.bfloat16)


MESH = pl.DeviceIdType.MESH
PAIR = 2
LINE = 4
LANES = 128
PARTS = 2
CROSS_IN = (-2.8, -5.5, -5.0, -1.9)


def moe_kernel(
    tokens_hbm, gain_hbm, router_hbm, ids_hbm, inner_hbm, outer_hbm, out_ref,
    tokens_ref, gain_ref, router_ref, ids_ref, inner_v, outer_v, ids_all, pick_own, place_own, pick_far, place_far,
    blocks, cross, pick_send, pick_recv, swap_send, rows, sums, hidden, gate,
    parts, core_recv, y_send, y_recv, kept, give, slots_v, raw, dense, dest_send, dest_recv,
    last_send, last_recv, last_own,
    w_sem, out_sem, ids_sem, x_sem, near_sem, far_sem, pick_sem, swap_sem, y_sem, c_sem, cr_sem,
    rc_sem, ry_sem, rx_sem, raw_sem, dest_sem, last_sem,
):
    chunks = blocks.shape[0]
    tok_rows = tokens_ref.shape[0]
    experts_dev, cap_dev = ids_ref.shape
    slots = experts_dev * cap_dev
    both = PAIR * tok_rows
    wide = PAIR * LANES
    pair_e = experts_dev // PARTS
    bf16, f32 = jnp.bfloat16, jnp.float32
    exp = lax.axis_index("exp")
    dat = lax.axis_index("dat")
    dat_count = lax.axis_size("dat")
    z, x = exp // PAIR, exp % PAIR
    y, c = dat // PAIR, dat % PAIR
    half = z // PAIR
    spot = z + half * (LINE - 1 - 2 * z)
    is_end = spot == 0
    is_inner = spot == 1

    def line_z(q):
        return q + half * (LINE - 1 - 2 * q)

    near = (line_z(1 - spot) * PAIR + x, dat)
    far_inner = (line_z(2) * PAIR + x, dat)
    far_end = (line_z(3) * PAIR + x, dat)
    x_peer = (exp + 1 - 2 * x, dat)
    y_peer = (exp, dat + PAIR - 2 * PAIR * y)
    c_peer = (exp, dat + 1 - 2 * c)
    near_diag = (line_z(1 - spot) * PAIR + 1 - x, dat)
    far_diag = (line_z(2) * PAIR + 1 - x, dat)
    far_end_diag = (line_z(3) * PAIR + 1 - x, dat)
    xy_diag = (exp + 1 - 2 * x, dat + PAIR - 2 * PAIR * y)
    last = chunks - 1

    def copy_to(src, dst, stage, sems, where, peer):
        return pltpu.make_async_remote_copy(
            src_ref=src, dst_ref=dst, send_sem=out_sem.at[stage],
            recv_sem=sems.at[where], device_id=peer, device_id_type=MESH,
        )

    def send(copy, cond=None):
        if cond is None:
            copy.start()
        else:
            pl.when(cond)(copy.start)

    loads = []
    for e in range(experts_dev):
        loads.append(pltpu.make_async_copy(inner_hbm.at[e], inner_v.at[e], w_sem.at[0]))
    for e in range(experts_dev):
        loads.append(pltpu.make_async_copy(outer_hbm.at[e], outer_v.at[e], w_sem.at[1]))
    inner_load = pltpu.make_async_copy(inner_hbm, inner_v, w_sem.at[0])
    outer_load = pltpu.make_async_copy(outer_hbm, outer_v, w_sem.at[1])

    barrier = pltpu.get_barrier_semaphore()
    for peer in (near, near_diag, far_inner, far_diag, x_peer, y_peer, xy_diag, c_peer):
        pl.semaphore_signal(barrier, inc=1, device_id=peer, device_id_type=MESH)

    @pl.when(is_inner)
    def _():
        for peer in (far_end, far_end_diag):
            pl.semaphore_signal(barrier, inc=1, device_id=peer, device_id_type=MESH)

    smalls = []
    for i, (src, dst) in enumerate(
        ((ids_hbm, ids_ref), (tokens_hbm, tokens_ref), (gain_hbm, gain_ref), (router_hbm, router_ref))
    ):
        smalls.append(pltpu.make_async_copy(src, dst, w_sem.at[2 + i]))
        smalls[i].start()
    for load in loads:
        load.start()
    smalls[1].wait()
    smalls[2].wait()

    values = tokens_ref[...].astype(f32)
    scale = lax.rsqrt(jnp.mean(values * values, axis=-1, keepdims=True) + EPSILON)
    normed = values * scale * gain_ref[...]

    def split(value):
        low, high = value[..., :LANES], value[..., LANES:]
        return jnp.where(x == 0, low, high), jnp.where(x == 0, high, low)

    for k in range(chunks):
        own, other = split(normed[:, k * wide : (k + 1) * wide])
        blocks[k, spot, 0] = own.astype(bf16)
        cross[k] = other.astype(bf16)

    def one_hots(ids, side, pick, place, first):
        row = jnp.concatenate([ids[e : e + 1, :] for e in range(experts_dev)], axis=1)
        column = jnp.broadcast_to(row, (LANES, slots)).T
        lane = lax.broadcasted_iota(jnp.int32, (slots, tok_rows), 1)
        line = lax.broadcasted_iota(jnp.int32, (tok_rows, slots), 0)
        at = slice(side * slots, (side + 1) * slots)
        for q in range(first, LINE):
            for xr in range(PAIR):
                x_of = x if xr == 0 else 1 - x
                base = ((line_z(q) * PAIR + x_of) * dat_count + dat) * tok_rows
                start = ((q - first) * PAIR + xr) * tok_rows
                span = slice(start, start + tok_rows)
                pick[at, span] = (column == lane + base).astype(f32).astype(bf16)
                place[span, at] = (row == line + base).astype(f32).astype(bf16)

    smalls[0].wait()
    one_hots(ids_ref, 0, pick_own, place_own, 0)

    pl.semaphore_wait(barrier, 8 + 2 * is_inner.astype(jnp.int32))

    def cross_copy(k):
        return copy_to(cross.at[k], blocks.at[k, spot, 1], 0, x_sem, (k,), x_peer)

    ids_x = copy_to(ids_ref, ids_all.at[1], 1, ids_sem, (0,), x_peer)
    ids_near = copy_to(ids_ref, ids_all.at[2], 2, ids_sem, (1,), near)
    ids_diag = copy_to(ids_ref, ids_all.at[3], 2, ids_sem, (1,), near_diag)
    ids_both = copy_to(ids_all.at[2:4], ids_all.at[2:4], 2, ids_sem, (1,), near)

    def near_copy(k, xr):
        ref = blocks.at[k, 0, xr]
        return copy_to(ref, ref, 3, near_sem, (k,), near)

    def far_copy(k, xr):
        return copy_to(blocks.at[k, spot, xr], blocks.at[k, 3 - spot, xr], 4, far_sem, (k,), far_inner)

    def block_send(k, xr):
        send(far_copy(k, xr))
        send(near_copy(k, xr), is_end)

    def diag_send(k):
        send(copy_to(cross.at[k], blocks.at[k, 3 - spot, 1], 4, far_sem, (k,), far_diag))
        send(copy_to(cross.at[k], blocks.at[k, 0, 1], 3, near_sem, (k,), near_diag), is_end)

    send(ids_x)
    send(ids_near, is_end)
    send(ids_diag, is_end)
    diag_send(0)
    block_send(0, 0)
    send(cross_copy(1))
    block_send(1, 0)
    send(cross_copy(0))
    block_send(2, 0)
    for k in range(2, chunks):
        send(cross_copy(k))

    def stage_cross_in(k):
        cross_copy(k).wait_recv()
        if k > 0:
            block_send(k, 1)
        if k == 1:
            for j in range(3, chunks):
                block_send(j, 0)

    def stage_ids():
        ids_x.wait_recv()
        one_hots(ids_all.at[1], 1, pick_own, place_own, 0)

        @pl.when(is_inner)
        def _():
            ids_both.wait_recv()
            one_hots(ids_all.at[2], 0, pick_far, place_far, 1)
            one_hots(ids_all.at[3], 1, pick_far, place_far, 1)

    def pair(p):
        return slice(p * pair_e, (p + 1) * pair_e)

    def own_rows(k, rel, p, of_dat):
        feature = k * PAIR + (x if rel == 0 else 1 - x)
        at = pl.ds(pl.multiple_of(of_dat * cap_dev, cap_dev), cap_dev)
        return rows.at[feature, pair(p), at]

    def dat_at(of_dat):
        return pl.ds(pl.multiple_of(of_dat * cap_dev, cap_dev), cap_dev)

    def pick_copy(k, xr, p):
        return copy_to(
            pick_send.at[k, xr, pair(p)], pick_recv.at[k, xr, pair(p)], 5, pick_sem, (k, xr, p), near
        )

    def swap_copy(k, p):
        return copy_to(
            swap_send.at[k, pair(p)], own_rows(k, 0, p, dat), 6, swap_sem, (k, p), x_peer
        )

    def far_swap(k, p):
        return copy_to(
            swap_send.at[k, pair(p)], own_rows(k, 0, p, dat), 7, y_sem, (k, 1, p), xy_diag
        )

    def y_copy(k, rel, p, of_dat):
        ref = own_rows(k, rel, p, of_dat)
        return copy_to(ref, ref, 7, y_sem, (k, rel, p), y_peer)

    def c_copy(k, rel, p, of_dat):
        ref = own_rows(k, rel, p, of_dat)
        return copy_to(ref, ref, 8, c_sem, (k, p), c_peer)

    def relay_copy(k, rel, p, of_dat):
        ref = own_rows(k, rel, p, of_dat)
        return copy_to(ref, ref, 9, cr_sem, (k, p), c_peer)

    def both_rows(k, p, of_dat):
        return rows.at[k * PAIR : (k + 1) * PAIR, pair(p), dat_at(of_dat)]

    dat_y = dat + PAIR - 2 * PAIR * y
    dat_c = dat + 1 - 2 * c
    dat_yc = dat_y + 1 - 2 * c

    def by_part(value):
        size = pair_e * cap_dev
        return [
            value[p * size : (p + 1) * size].reshape(pair_e, cap_dev, LANES) for p in range(PARTS)
        ]

    def sides(k):
        return (1, 0) if k + 1 == chunks else (0, 1)

    def stage_far_pick(k):
        @pl.when(is_inner)
        def _():
            near_all, far_all = blocks.at[k, 0], blocks.at[k, 2:4]
            copy_to(near_all, near_all, 3, near_sem, (k,), near).wait_recv()
            copy_to(far_all, far_all, 4, far_sem, (k,), far_inner).wait_recv()
            found = blocks[k].reshape(LINE * both, LANES)
            for xr in sides(k):
                at = slice(xr * slots, (xr + 1) * slots)
                got = jnp.dot(pick_far[at, :], found[both:], preferred_element_type=f32)
                got = by_part(got.astype(bf16))
                for p in range(PARTS):
                    pick_send[k, xr, pair(p)] = got[p]
                    pick_copy(k, xr, p).start()

    def hand_on(k, xr, p, value):
        if xr == 1:
            swap_send[k, pair(p)] = value
            swap_copy(k, p).start()
            far_swap(k, p).start()
        else:
            own_rows(k, 0, p, dat)[...] = value
            y_copy(k, 0, p, dat).start()
            c_copy(k, 0, p, dat).start()

    def stage_pick(k):
        @pl.when(is_inner)
        def _():
            found = blocks[k].reshape(LINE * both, LANES)
            for xr in (1, 0):
                at = slice(xr * slots, (xr + 1) * slots)
                got = jnp.dot(pick_own[at, :], found, preferred_element_type=f32)
                got = by_part(got.astype(bf16))
                for p in range(PARTS):
                    hand_on(k, xr, p, got[p])

        @pl.when(is_end)
        def _():
            found = blocks[k, 0].reshape(both, LANES)
            for xr in sides(k):
                at = slice(xr * slots, (xr + 1) * slots)
                got = by_part(jnp.dot(pick_own[at, :both], found, preferred_element_type=f32))
                for p in range(PARTS):
                    pick_copy(k, xr, p).wait_recv()
                    here = got[p] + pick_recv[k, xr, pair(p)].astype(f32)
                    hand_on(k, xr, p, here.astype(bf16))

    def stage_swap(k):
        for p in range(PARTS):
            ref = own_rows(k, 1, p, dat)
            copy_to(ref, ref, 6, swap_sem, (k, p), x_peer).wait_recv()
            send(c_copy(k, 1, p, dat))

    def stage_relay(k, rel):
        for p in range(PARTS):
            y_copy(k, rel, p, dat_y).wait_recv()
            send(relay_copy(k, rel, p, dat_y))

    def stage_first(k, p):
        for sems, stage, of_dat in ((c_sem, 8, dat_c), (cr_sem, 9, dat_yc)):
            ref = both_rows(k, p, of_dat)
            copy_to(ref, ref, stage, sems, (k, p), c_peer).wait_recv()
        if k == 0 and p == 0:
            inner_load.wait()

        for e in range(p * pair_e, (p + 1) * pair_e):
            left = jnp.concatenate([rows[PAIR * k, e], rows[PAIR * k + 1, e]], axis=1)
            total = jnp.dot(left, inner_v[e, k * wide : (k + 1) * wide, :], preferred_element_type=f32)
            if k > 0:
                total += sums[e]
            if k + 1 < chunks:
                sums[e] = total
            else:
                hidden[e] = jnp.maximum(total, 0.0).astype(bf16)

    def core_copy(k, p):
        return copy_to(
            parts.at[k, :, 1 - c, pair(p)], core_recv.at[k, :, pair(p)], 10, rc_sem, (k, p), c_peer
        )

    def back_y(k, p):
        return copy_to(y_send.at[k, pair(p)], y_recv.at[k, pair(p)], 11, ry_sem, (k, p), y_peer)

    def back_x(k, p):
        return copy_to(give.at[k, pair(p)], slots_v.at[k, 1, pair(p)], 12, rx_sem, (k, p), x_peer)

    def raw_copy(k, xr, p):
        return copy_to(
            slots_v.at[k, xr, pair(p)], raw.at[k, xr, pair(p)], 13, raw_sem, (k,), near
        )

    def dest_copy(k, j, xr, peer):
        return copy_to(
            dest_send.at[k, j, xr], dest_recv.at[k, min(j, 1), xr], 14, dest_sem, (k, xr), peer
        )

    def last_copy(k):
        return copy_to(last_send.at[k], last_recv.at[k], 15, last_sem, (k,), x_peer)

    def stage_second(k, p):
        if k == 0 and p == 0:
            outer_load.wait()
        for e in range(p * pair_e, (p + 1) * pair_e):
            part = jnp.dot(
                hidden[e], outer_v[e, :, k * wide : (k + 1) * wide], preferred_element_type=f32
            ).astype(bf16)
            for d in range(PAIR * PAIR):
                parts[k, d // PAIR, d % PAIR, e] = part[d * cap_dev : (d + 1) * cap_dev]
        send(core_copy(k, p))

    def stage_core(k, p):
        core_copy(k, p).wait_recv()
        theirs = parts[k, 1 - y, c, pair(p)].astype(f32) + core_recv[k, 1 - y, pair(p)].astype(f32)
        y_send[k, pair(p)] = theirs.astype(bf16)
        send(back_y(k, p))
        ours = parts[k, y, c, pair(p)].astype(f32) + core_recv[k, y, pair(p)].astype(f32)
        kept[k, pair(p)] = ours

    def gates():
        smalls[3].wait()
        at = pl.ds(pl.multiple_of(dat * cap_dev, cap_dev), cap_dev)
        for e in range(experts_dev):
            score = jnp.zeros((cap_dev, LANES), f32)
            for b in range(PAIR * chunks):
                weight = router_ref[e : e + 1, b * LANES : (b + 1) * LANES].astype(f32)
                score += rows[b, e, at].astype(f32) * weight
            gate[e] = jax.nn.sigmoid(jnp.sum(score, axis=-1, keepdims=True))

    def stage_weigh(k, p):
        back_y(k, p).wait_recv()
        summed = kept[k, pair(p)] + y_recv[k, pair(p)].astype(f32)
        own, other = split(gate[pair(p)] * summed)
        give[k, pair(p)] = other.astype(bf16)
        ref = raw.at[k, 1, pair(p)]
        send(copy_to(give.at[k, pair(p)], ref, 13, raw_sem, (k,), near_diag), is_end)
        send(back_x(k, p))
        slots_v[k, 0, pair(p)] = own.astype(bf16)
        send(raw_copy(k, 0, p), is_end)

    def stage_cross(k, p):
        back_x(k, p).wait_recv()

    def dest_out(k, j, total, peer, peer_diag):
        for xr in (1, 0):
            dest_send[k, j, xr] = total[xr * tok_rows : (xr + 1) * tok_rows].astype(bf16)
            dest_copy(k, j, xr, peer_diag if k == last and xr == 1 else peer).start()

    def last_out(k, total):
        last_send[k] = total.astype(bf16)
        last_copy(k).start()

    def stage_place(k):
        held = slots_v[k].reshape(PAIR * slots, LANES)

        @pl.when(is_inner)
        def _():
            dest_out(k, 0, jnp.dot(place_own[:both, :], held, preferred_element_type=f32), near, near_diag)

        at = pl.ds(pl.multiple_of(spot * both, both), both)
        total = jnp.dot(place_own[at, :], held, preferred_element_type=f32)
        dense[k] = total
        if k == last:

            @pl.when(is_end)
            def _():
                last_out(k, total[tok_rows:])

    def stage_far(k):
        @pl.when(is_inner)
        def _():
            held = slots_v[k].reshape(PAIR * slots, LANES)
            mine = jnp.dot(place_own[2 * both :, :], held, preferred_element_type=f32)
            copy_to(raw.at[k], raw.at[k], 13, raw_sem, (k,), near).wait_recv()
            ends = raw[k].reshape(PAIR * slots, LANES)
            mine += jnp.dot(place_far[both:, :], ends, preferred_element_type=f32)
            dest_out(k, 2, mine[both:], far_end, far_end_diag)
            dest_out(k, 1, mine[:both], far_inner, far_diag)
            total = dense[k] + jnp.dot(place_far[:both, :], ends, preferred_element_type=f32)
            dense[k] = total
            if k == last:
                last_out(k, total[tok_rows:])

    def arrived(k, xr, ref):
        copy_to(ref, ref, 14, dest_sem, (k, xr), near).wait_recv()

    def stage_total(k):
        def finish(total, xr):
            if xr == 1:
                last_out(k, total)
            else:
                last_own[k] = total

        where = (0,) if k == last else (1, 0)

        @pl.when(is_end)
        def _():
            for xr in where:
                arrived(k, xr, dest_recv.at[k, :, xr])
                held = dense[k, xr * tok_rows : (xr + 1) * tok_rows]
                finish(held + dest_recv[k, 0, xr].astype(f32) + dest_recv[k, 1, xr].astype(f32), xr)

        @pl.when(is_inner)
        def _():
            for xr in where:
                arrived(k, xr, dest_recv.at[k, 1, xr])
                held = dense[k, xr * tok_rows : (xr + 1) * tok_rows]
                finish(held + dest_recv[k, 1, xr].astype(f32), xr)

    def stage_last(k):
        def finish(own, other):
            cols = slice(k * wide, (k + 1) * wide)
            left, right = jnp.where(x == 0, own, other), jnp.where(x == 0, other, own)
            total = jnp.concatenate([left, right], axis=1)
            out_ref[:, cols] = (tokens_ref[:, cols].astype(f32) + total).astype(bf16)

        last_copy(k).wait_recv()
        own, other = last_own[k], last_recv[k].astype(f32)
        if k < last:
            finish(own, other)
            return

        @pl.when(is_end)
        def _():
            arrived(k, 1, dest_recv.at[k, :, 1])
            finish(own, other + dest_recv[k, 0, 1].astype(f32) + dest_recv[k, 1, 1].astype(f32))

        @pl.when(is_inner)
        def _():
            arrived(k, 1, dest_recv.at[k, 1, 1])
            finish(own, other + dest_recv[k, 1, 1].astype(f32))

    def run_first(k):
        for p in range(PARTS):
            stage_first(k, p)
            if k == last:
                stage_second(0, p)

    order = [(-6.0, stage_ids, ())]
    for k in range(chunks):
        order += [
            (CROSS_IN[k], stage_cross_in, (k,)),
            (2.8 * k - 2.65, stage_far_pick, (k,)),
            (2.8 * k, stage_pick, (k,)),
            (2.8 * k + 3.1, stage_swap, (k,)),
            (2.8 * k + 3.9, stage_relay, (k, 0)),
            (2.8 * k + 7.0, stage_relay, (k, 1)),
            (2.8 * k + 8.9, run_first, (k,)),
        ]
    for _, stage, where in sorted(order, key=lambda step: step[0]):
        stage(*where)

    pieces = [(k, p) for k in range(chunks) for p in range(PARTS)]
    for i in range(PARTS, len(pieces)):
        stage_second(*pieces[i])
        stage_core(*pieces[i - PARTS])
    gates()
    for i in range(len(pieces) - PARTS, len(pieces)):
        stage_core(*pieces[i])

    order = []
    for k in range(chunks):
        order += [
            (2 * k + 0.0, stage_weigh, (k, 0)),
            (2 * k + 1.0, stage_weigh, (k, 1)),
            (2 * k + 2.1, stage_cross, (k, 0)),
            (2 * k + 3.1, stage_cross, (k, 1)),
            (2 * k + 3.2, stage_place, (k,)),
            (2 * k + 7.05, stage_far, (k,)),
            (2 * k + 11.4, stage_total, (k,)),
            (2 * k + 15.6, stage_last, (k,)),
        ]
    for _, stage, where in sorted(order, key=lambda step: step[0]):
        stage(*where)

    def sent(ref, stage, cond=None):
        done = copy_to(ref, ref, stage, ids_sem, (0,), x_peer)
        if cond is None:
            done.wait_send()
        else:
            pl.when(cond)(done.wait_send)

    own_all = rows.at[:, :, dat_at(dat)]
    sent(cross, 0)
    sent(ids_ref, 1)
    sent(ids_all.at[2:4], 2, is_end)
    sent(blocks.at[0], 3, is_end)
    sent(blocks.at[0], 4)
    sent(pick_send, 5, is_inner)
    sent(swap_send, 6)
    for stage in (7, 8, 9):
        sent(own_all, stage)
    sent(parts.at[:, :, 1 - c], 10)
    sent(y_send, 11)
    sent(give, 12)
    sent(slots_v, 13, is_end)
    sent(dest_send, 14, is_inner)
    sent(last_send, 15)


def kernel_body(tokens, norm_gain, router_weight, inner_weight, outer_weight, slot_tokens, slot_ids):
    del slot_ids
    tok_rows, width = tokens.shape
    experts_dev, cap_dev = slot_tokens.shape
    units = inner_weight.shape[2]
    dat_count = lax.axis_size("dat")
    slots = experts_dev * cap_dev
    wide = PAIR * LANES
    chunks = width // wide
    both = PAIR * tok_rows
    bf16, f32 = jnp.bfloat16, jnp.float32
    vmem = pl.BlockSpec(memory_space=pltpu.VMEM)
    hbm = pl.BlockSpec(memory_space=pltpu.HBM)
    dma = pltpu.SemaphoreType.DMA

    def buffer(*shape, kind=bf16):
        return pltpu.VMEM(shape, kind)

    return pl.pallas_call(
        moe_kernel,
        out_shape=jax.ShapeDtypeStruct((tok_rows, width), bf16),
        in_specs=[hbm] * 6,
        out_specs=vmem,
        scratch_shapes=[
            buffer(tok_rows, width),
            buffer(1, width, kind=f32),
            buffer(experts_dev, width),
            buffer(experts_dev, cap_dev, kind=jnp.int32),
            buffer(experts_dev, width, units),
            buffer(experts_dev, units, width),
            buffer(LINE, experts_dev, cap_dev, kind=jnp.int32),
            buffer(PAIR * slots, LINE * both),
            buffer(LINE * both, PAIR * slots),
            buffer(PAIR * slots, (LINE - 1) * both),
            buffer((LINE - 1) * both, PAIR * slots),
            buffer(chunks, LINE, PAIR, tok_rows, LANES),
            buffer(chunks, tok_rows, LANES),
            buffer(chunks, PAIR, experts_dev, cap_dev, LANES),
            buffer(chunks, PAIR, experts_dev, cap_dev, LANES),
            buffer(chunks, experts_dev, cap_dev, LANES),
            buffer(PAIR * chunks, experts_dev, dat_count * cap_dev, LANES),
            buffer(experts_dev, dat_count * cap_dev, units, kind=f32),
            buffer(experts_dev, dat_count * cap_dev, units),
            buffer(experts_dev, cap_dev, 1, kind=f32),
            buffer(chunks, PAIR, PAIR, experts_dev, cap_dev, wide),
            buffer(chunks, PAIR, experts_dev, cap_dev, wide),
            buffer(chunks, experts_dev, cap_dev, wide),
            buffer(chunks, experts_dev, cap_dev, wide),
            buffer(chunks, experts_dev, cap_dev, wide, kind=f32),
            buffer(chunks, experts_dev, cap_dev, LANES),
            buffer(chunks, PAIR, experts_dev, cap_dev, LANES),
            buffer(chunks, PAIR, experts_dev, cap_dev, LANES),
            buffer(chunks, both, LANES, kind=f32),
            buffer(chunks, LINE - 1, PAIR, tok_rows, LANES),
            buffer(chunks, 2, PAIR, tok_rows, LANES),
            buffer(chunks, tok_rows, LANES),
            buffer(chunks, tok_rows, LANES),
            buffer(chunks, tok_rows, LANES, kind=f32),
            dma((6,)),
            dma((16,)),
            dma((2,)),
            dma((chunks,)),
            dma((chunks,)),
            dma((chunks,)),
            dma((chunks, PAIR, PARTS)),
            dma((chunks, PARTS)),
            dma((chunks, PAIR, PARTS)),
            dma((chunks, PARTS)),
            dma((chunks, PARTS)),
            dma((chunks, PARTS)),
            dma((chunks, PARTS)),
            dma((chunks, PARTS)),
            dma((chunks,)),
            dma((chunks, PAIR)),
            dma((chunks,)),
        ],
        compiler_params=pltpu.CompilerParams(
            collective_id=0, has_side_effects=True, vmem_limit_bytes=48 * 1024 * 1024
        ),
    )(
        *(
            pltpu.with_memory_space_constraint(array, pltpu.HBM)
            for array in (tokens, norm_gain.reshape(1, width), router_weight.T, slot_tokens)
        ),
        inner_weight,
        outer_weight,
    )


def solution(mesh):
    fits = mesh.shape["dat"] == PAIR * PAIR and mesh.shape["exp"] == PAIR * LINE
    chosen = kernel_body if fits else body
    in_specs = (
        P(("exp", "dat"), None),
        P(),
        P(None, "exp"),
        P("exp", None, "dat"),
        P("exp", "dat", None),
        P("exp", "dat"),
        P(("exp", "dat"), None),
    )
    out_specs = P(("exp", "dat"), None)
    return jax.shard_map(chosen, mesh=mesh, in_specs=in_specs, out_specs=out_specs, check_vma=False)
```

```python
import jax
import jax.numpy as jnp
from jax import lax
from jax.experimental import pallas as pl
from jax.experimental.pallas import tpu as pltpu
from jax.sharding import PartitionSpec as P

EPSILON = 1e-06


def normalize(tokens, norm_gain):
    values = tokens.astype(jnp.float32)
    scale = lax.rsqrt(jnp.mean(values * values, axis=-1, keepdims=True) + EPSILON)
    return (values * scale * norm_gain).astype(jnp.bfloat16)


def owner_places(slot_ids, experts_dev, capacity, bucket):
    flat_ids = slot_ids.reshape(-1)
    source = flat_ids // capacity // experts_dev
    before = (source[:, None] == source[None, :]) & (flat_ids[None, :] < flat_ids[:, None])
    ranks_in = jnp.sum(before.astype(jnp.int32), axis=1)
    return (source * bucket + ranks_in).reshape(slot_ids.shape)


def expert_places(token_ids, slot_keys, tok_rows, dat_count, bucket):
    owner_of = token_ids // (tok_rows * dat_count)
    before = (owner_of[:, None] == owner_of[None, :]) & (slot_keys[None, :] < slot_keys[:, None])
    ranks_in = jnp.sum(before.astype(jnp.int32), axis=1)
    return owner_of * bucket + ranks_in


def body(tokens, norm_gain, router_weight, inner_weight, outer_weight, slot_tokens, slot_ids):
    exp_count = lax.axis_size("exp")
    dat_count = lax.axis_size("dat")
    tok_rows, width = tokens.shape
    experts_dev, cap_dev = slot_tokens.shape
    bucket = 6 * tok_rows // exp_count
    normed = normalize(tokens, norm_gain)
    picked = slot_tokens.T.reshape(-1)
    expert_iota = lax.broadcasted_iota(jnp.int32, (cap_dev, experts_dev), 1)
    column_iota = lax.broadcasted_iota(jnp.int32, (cap_dev, experts_dev), 0)
    slot_keys = (expert_iota * cap_dev + column_iota).reshape(-1)
    senders = expert_places(picked, slot_keys, tok_rows, dat_count, bucket)
    receivers = owner_places(slot_ids, experts_dev, cap_dev * dat_count, bucket)
    lookup = jnp.any(
        lax.broadcasted_iota(jnp.int32, (exp_count * bucket, 1, 1), 0) == receivers[None], axis=2
    )
    outgoing = jnp.dot(lookup.astype(jnp.bfloat16), normed, preferred_element_type=jnp.float32)
    outgoing = outgoing.astype(jnp.bfloat16).reshape(exp_count, bucket, width)
    arrived = lax.all_to_all(outgoing, "exp", split_axis=0, concat_axis=0, tiled=True).reshape(
        exp_count * bucket, width
    )
    gathered_rows = jnp.take(arrived, senders, axis=0)
    gathered_rows = gathered_rows.reshape(cap_dev, experts_dev, width)
    gate_score = jax.nn.sigmoid(
        jnp.einsum("ced,de->ce", gathered_rows, router_weight, preferred_element_type=jnp.float32)
    )
    inner = jnp.einsum(
        "ced,edf->cef",
        lax.all_gather(gathered_rows, "dat", axis=0, tiled=True),
        inner_weight,
        preferred_element_type=jnp.float32,
    )
    hidden = jax.nn.relu(inner).astype(jnp.bfloat16)
    expert_out = lax.psum_scatter(
        jnp.einsum("cef,efd->ced", hidden, outer_weight, preferred_element_type=jnp.float32).astype(
            jnp.bfloat16
        ),
        "dat",
        scatter_dimension=0,
        tiled=True,
    ).astype(jnp.float32)
    weighted = (gate_score[:, :, None] * expert_out).astype(jnp.bfloat16).reshape(-1, width)
    placing = lax.broadcasted_iota(jnp.int32, (exp_count * bucket, 1), 0) == senders[None, :]
    returning = jnp.dot(placing.astype(jnp.bfloat16), weighted, preferred_element_type=jnp.float32)
    returning = returning.astype(jnp.bfloat16).reshape(exp_count, bucket, width)
    came_back = lax.all_to_all(returning, "exp", split_axis=0, concat_axis=0, tiled=True).reshape(
        exp_count * bucket, width
    )
    combine_table = jnp.sum(
        (
            lax.broadcasted_iota(jnp.int32, (1, 1, exp_count * bucket), 2) == receivers[:, :, None]
        ).astype(jnp.float32),
        axis=1,
    )
    combined = jnp.dot(
        combine_table.astype(jnp.bfloat16), came_back, preferred_element_type=jnp.float32
    )
    return (tokens.astype(jnp.float32) + combined).astype(jnp.bfloat16)


MESH = pl.DeviceIdType.MESH
PAIR = 2
LINE = 4
LANES = 128
PARTS = 2
FIRST_AT = (9.6, 11.3, 14.5, 16.8)
RELAY_AT = (5.65, 8.45, 11.25, 12.4)
CROSS_IN = (-5.5, -5.4, -2.6, -1.9)


def moe_kernel(
    tokens_hbm, gain_hbm, router_hbm, ids_hbm, inner_hbm, outer_hbm, out_ref,
    tokens_ref, gain_ref, router_ref, ids_ref, inner_v, outer_v, ids_all, pick_own, place_own, pick_far, place_far,
    blocks, cross, pick_send, pick_recv, swap_send, rows, sums, hidden, gate,
    parts, core_recv, y_send, y_recv, kept, give, slots_v, raw, dense, dest_send, dest_recv,
    last_send, last_recv, last_own,
    w_sem, out_sem, ids_sem, x_sem, near_sem, far_sem, pick_sem, swap_sem, y_sem, c_sem, cr_sem,
    rc_sem, ry_sem, rx_sem, raw_sem, dest_sem, last_sem,
):
    chunks = blocks.shape[0]
    tok_rows = tokens_ref.shape[0]
    experts_dev, cap_dev = ids_ref.shape
    slots = experts_dev * cap_dev
    both = PAIR * tok_rows
    wide = PAIR * LANES
    pair_e = experts_dev // PARTS
    bf16, f32 = jnp.bfloat16, jnp.float32
    exp = lax.axis_index("exp")
    dat = lax.axis_index("dat")
    dat_count = lax.axis_size("dat")
    z, x = exp // PAIR, exp % PAIR
    y, c = dat // PAIR, dat % PAIR
    half = z // PAIR
    spot = z + half * (LINE - 1 - 2 * z)
    is_end = spot == 0
    is_inner = spot == 1

    def line_z(q):
        return q + half * (LINE - 1 - 2 * q)

    near = (line_z(1 - spot) * PAIR + x, dat)
    far_inner = (line_z(2) * PAIR + x, dat)
    far_end = (line_z(3) * PAIR + x, dat)
    x_peer = (exp + 1 - 2 * x, dat)
    y_peer = (exp, dat + PAIR - 2 * PAIR * y)
    c_peer = (exp, dat + 1 - 2 * c)
    near_diag = (line_z(1 - spot) * PAIR + 1 - x, dat)
    far_diag = (line_z(2) * PAIR + 1 - x, dat)
    far_end_diag = (line_z(3) * PAIR + 1 - x, dat)
    xy_diag = (exp + 1 - 2 * x, dat + PAIR - 2 * PAIR * y)
    last = chunks - 1

    def copy_to(src, dst, stage, sems, where, peer):
        return pltpu.make_async_remote_copy(
            src_ref=src, dst_ref=dst, send_sem=out_sem.at[stage],
            recv_sem=sems.at[where], device_id=peer, device_id_type=MESH,
        )

    def send(copy, cond=None):
        if cond is None:
            copy.start()
        else:
            pl.when(cond)(copy.start)

    loads = []
    for e in range(experts_dev):
        loads.append(pltpu.make_async_copy(inner_hbm.at[e], inner_v.at[e], w_sem.at[0]))
    for e in range(experts_dev):
        loads.append(pltpu.make_async_copy(outer_hbm.at[e], outer_v.at[e], w_sem.at[1]))
    inner_load = pltpu.make_async_copy(inner_hbm, inner_v, w_sem.at[0])
    outer_load = pltpu.make_async_copy(outer_hbm, outer_v, w_sem.at[1])

    barrier = pltpu.get_barrier_semaphore()
    for peer in (near, near_diag, far_inner, far_diag, x_peer, y_peer, xy_diag, c_peer):
        pl.semaphore_signal(barrier, inc=1, device_id=peer, device_id_type=MESH)

    @pl.when(is_inner)
    def _():
        for peer in (far_end, far_end_diag):
            pl.semaphore_signal(barrier, inc=1, device_id=peer, device_id_type=MESH)

    smalls = []
    for i, (src, dst) in enumerate(
        ((ids_hbm, ids_ref), (tokens_hbm, tokens_ref), (gain_hbm, gain_ref), (router_hbm, router_ref))
    ):
        smalls.append(pltpu.make_async_copy(src, dst, w_sem.at[2 + i]))
        smalls[i].start()
    for load in loads:
        load.start()
    smalls[1].wait()
    smalls[2].wait()

    values = tokens_ref[...].astype(f32)
    scale = lax.rsqrt(jnp.mean(values * values, axis=-1, keepdims=True) + EPSILON)
    normed = values * scale * gain_ref[...]

    def split(value):
        low, high = value[..., :LANES], value[..., LANES:]
        return jnp.where(x == 0, low, high), jnp.where(x == 0, high, low)

    for k in range(chunks):
        own, other = split(normed[:, k * wide : (k + 1) * wide])
        blocks[k, spot, 0] = own.astype(bf16)
        cross[k] = other.astype(bf16)

    def one_hots(ids, side, pick, place, first):
        row = jnp.concatenate([ids[e : e + 1, :] for e in range(experts_dev)], axis=1)
        column = jnp.broadcast_to(row, (LANES, slots)).T
        lane = lax.broadcasted_iota(jnp.int32, (slots, tok_rows), 1)
        line = lax.broadcasted_iota(jnp.int32, (tok_rows, slots), 0)
        at = slice(side * slots, (side + 1) * slots)
        for q in range(first, LINE):
            for xr in range(PAIR):
                x_of = x if xr == 0 else 1 - x
                base = ((line_z(q) * PAIR + x_of) * dat_count + dat) * tok_rows
                start = ((q - first) * PAIR + xr) * tok_rows
                span = slice(start, start + tok_rows)
                pick[at, span] = (column == lane + base).astype(f32).astype(bf16)
                place[span, at] = (row == line + base).astype(f32).astype(bf16)

    smalls[0].wait()
    one_hots(ids_ref, 0, pick_own, place_own, 0)

    pl.semaphore_wait(barrier, 8 + 2 * is_inner.astype(jnp.int32))

    def cross_copy(k):
        return copy_to(cross.at[k], blocks.at[k, spot, 1], 0, x_sem, (k,), x_peer)

    ids_x = copy_to(ids_ref, ids_all.at[1], 1, ids_sem, (0,), x_peer)
    ids_near = copy_to(ids_ref, ids_all.at[2], 2, ids_sem, (1,), near)
    ids_diag = copy_to(ids_ref, ids_all.at[3], 2, ids_sem, (1,), near_diag)
    ids_both = copy_to(ids_all.at[2:4], ids_all.at[2:4], 2, ids_sem, (1,), near)

    def near_copy(k, xr):
        ref = blocks.at[k, 0, xr]
        return copy_to(ref, ref, 3, near_sem, (k,), near)

    def far_copy(k, xr):
        return copy_to(blocks.at[k, spot, xr], blocks.at[k, 3 - spot, xr], 4, far_sem, (k,), far_inner)

    def block_send(k, xr):
        send(far_copy(k, xr))
        send(near_copy(k, xr), is_end)

    def diag_send(k):
        send(copy_to(cross.at[k], blocks.at[k, 3 - spot, 1], 4, far_sem, (k,), far_diag))
        send(copy_to(cross.at[k], blocks.at[k, 0, 1], 3, near_sem, (k,), near_diag), is_end)

    send(ids_x)
    send(ids_near, is_end)
    send(ids_diag, is_end)
    send(cross_copy(0))
    diag_send(0)
    block_send(0, 0)
    send(cross_copy(1))
    block_send(1, 0)
    block_send(2, 0)
    for k in range(2, chunks):
        send(cross_copy(k))

    def stage_cross_in(k):
        cross_copy(k).wait_recv()
        if k > 0:
            block_send(k, 1)
        if k == 1:
            for j in range(3, chunks):
                block_send(j, 0)

    def stage_ids():
        ids_x.wait_recv()
        one_hots(ids_all.at[1], 1, pick_own, place_own, 0)

        @pl.when(is_inner)
        def _():
            ids_both.wait_recv()
            one_hots(ids_all.at[2], 0, pick_far, place_far, 1)
            one_hots(ids_all.at[3], 1, pick_far, place_far, 1)

    def pair(p):
        return slice(p * pair_e, (p + 1) * pair_e)

    def own_rows(k, rel, p, of_dat):
        feature = k * PAIR + (x if rel == 0 else 1 - x)
        at = pl.ds(pl.multiple_of(of_dat * cap_dev, cap_dev), cap_dev)
        return rows.at[feature, pair(p), at]

    def dat_at(of_dat):
        return pl.ds(pl.multiple_of(of_dat * cap_dev, cap_dev), cap_dev)

    def pick_copy(k, xr, p):
        return copy_to(
            pick_send.at[k, xr, pair(p)], pick_recv.at[k, xr, pair(p)], 5, pick_sem, (k, xr, p), near
        )

    def swap_copy(k, p):
        return copy_to(
            swap_send.at[k, pair(p)], own_rows(k, 0, p, dat), 6, swap_sem, (k, p), x_peer
        )

    def far_swap(k, p):
        return copy_to(
            swap_send.at[k, pair(p)], own_rows(k, 0, p, dat), 7, y_sem, (k, 1, p), xy_diag
        )

    def y_copy(k, rel, p, of_dat):
        ref = own_rows(k, rel, p, of_dat)
        return copy_to(ref, ref, 7, y_sem, (k, rel, p), y_peer)

    def c_copy(k, rel, p, of_dat):
        ref = own_rows(k, rel, p, of_dat)
        return copy_to(ref, ref, 8, c_sem, (k, p), c_peer)

    def relay_copy(k, rel, p, of_dat):
        ref = own_rows(k, rel, p, of_dat)
        return copy_to(ref, ref, 9, cr_sem, (k, p), c_peer)

    def both_rows(k, p, of_dat):
        return rows.at[k * PAIR : (k + 1) * PAIR, pair(p), dat_at(of_dat)]

    dat_y = dat + PAIR - 2 * PAIR * y
    dat_c = dat + 1 - 2 * c
    dat_yc = dat_y + 1 - 2 * c

    def by_part(value):
        size = pair_e * cap_dev
        return [
            value[p * size : (p + 1) * size].reshape(pair_e, cap_dev, LANES) for p in range(PARTS)
        ]

    def sides(k):
        return (1, 0) if k + 1 == chunks else (0, 1)

    def stage_far_pick(k):
        @pl.when(is_inner)
        def _():
            near_all, far_all = blocks.at[k, 0], blocks.at[k, 2:4]
            copy_to(near_all, near_all, 3, near_sem, (k,), near).wait_recv()
            copy_to(far_all, far_all, 4, far_sem, (k,), far_inner).wait_recv()
            found = blocks[k].reshape(LINE * both, LANES)
            for xr in sides(k):
                at = slice(xr * slots, (xr + 1) * slots)
                got = jnp.dot(pick_far[at, :], found[both:], preferred_element_type=f32)
                got = by_part(got.astype(bf16))
                for p in range(PARTS):
                    pick_send[k, xr, pair(p)] = got[p]
                    pick_copy(k, xr, p).start()

    def hand_on(k, xr, p, value):
        if xr == 1:
            swap_send[k, pair(p)] = value
            swap_copy(k, p).start()
            far_swap(k, p).start()
        else:
            own_rows(k, 0, p, dat)[...] = value
            y_copy(k, 0, p, dat).start()
            c_copy(k, 0, p, dat).start()

    def stage_pick(k):
        @pl.when(is_inner)
        def _():
            found = blocks[k].reshape(LINE * both, LANES)
            for xr in (1, 0):
                at = slice(xr * slots, (xr + 1) * slots)
                got = jnp.dot(pick_own[at, :], found, preferred_element_type=f32)
                got = by_part(got.astype(bf16))
                for p in range(PARTS):
                    hand_on(k, xr, p, got[p])

        @pl.when(is_end)
        def _():
            found = blocks[k, 0].reshape(both, LANES)
            for xr in sides(k):
                at = slice(xr * slots, (xr + 1) * slots)
                got = by_part(jnp.dot(pick_own[at, :both], found, preferred_element_type=f32))
                for p in range(PARTS):
                    pick_copy(k, xr, p).wait_recv()
                    here = got[p] + pick_recv[k, xr, pair(p)].astype(f32)
                    hand_on(k, xr, p, here.astype(bf16))

    def stage_swap(k):
        for p in range(PARTS):
            ref = own_rows(k, 1, p, dat)
            copy_to(ref, ref, 6, swap_sem, (k, p), x_peer).wait_recv()
            send(c_copy(k, 1, p, dat))

    def stage_relay(k, rel):
        for p in range(PARTS):
            y_copy(k, rel, p, dat_y).wait_recv()
            send(relay_copy(k, rel, p, dat_y))

    def stage_first(k, p):
        for sems, stage, of_dat in ((c_sem, 8, dat_c), (cr_sem, 9, dat_yc)):
            ref = both_rows(k, p, of_dat)
            copy_to(ref, ref, stage, sems, (k, p), c_peer).wait_recv()
        if k == 0 and p == 0:
            inner_load.wait()

        for e in range(p * pair_e, (p + 1) * pair_e):
            left = jnp.concatenate([rows[PAIR * k, e], rows[PAIR * k + 1, e]], axis=1)
            total = jnp.dot(left, inner_v[e, k * wide : (k + 1) * wide, :], preferred_element_type=f32)
            if k > 0:
                total += sums[e]
            if k + 1 < chunks:
                sums[e] = total
            else:
                hidden[e] = jnp.maximum(total, 0.0).astype(bf16)

    def core_copy(k, p):
        return copy_to(
            parts.at[k, :, 1 - c, pair(p)], core_recv.at[k, :, pair(p)], 10, rc_sem, (k, p), c_peer
        )

    def back_y(k, p):
        return copy_to(y_send.at[k, pair(p)], y_recv.at[k, pair(p)], 11, ry_sem, (k, p), y_peer)

    def back_x(k, p):
        return copy_to(give.at[k, pair(p)], slots_v.at[k, 1, pair(p)], 12, rx_sem, (k, p), x_peer)

    def raw_copy(k, xr, p):
        return copy_to(
            slots_v.at[k, xr, pair(p)], raw.at[k, xr, pair(p)], 13, raw_sem, (k,), near
        )

    def dest_copy(k, j, xr, peer):
        return copy_to(
            dest_send.at[k, j, xr], dest_recv.at[k, min(j, 1), xr], 14, dest_sem, (k, xr), peer
        )

    def last_copy(k):
        return copy_to(last_send.at[k], last_recv.at[k], 15, last_sem, (k,), x_peer)

    def stage_second(k, p):
        if k == 0 and p == 0:
            outer_load.wait()
        for e in range(p * pair_e, (p + 1) * pair_e):
            part = jnp.dot(
                hidden[e], outer_v[e, :, k * wide : (k + 1) * wide], preferred_element_type=f32
            ).astype(bf16)
            for d in range(PAIR * PAIR):
                parts[k, d // PAIR, d % PAIR, e] = part[d * cap_dev : (d + 1) * cap_dev]
        send(core_copy(k, p))

    def stage_core(k, p):
        core_copy(k, p).wait_recv()
        theirs = parts[k, 1 - y, c, pair(p)].astype(f32) + core_recv[k, 1 - y, pair(p)].astype(f32)
        y_send[k, pair(p)] = theirs.astype(bf16)
        send(back_y(k, p))
        ours = parts[k, y, c, pair(p)].astype(f32) + core_recv[k, y, pair(p)].astype(f32)
        kept[k, pair(p)] = ours

    def gates():
        smalls[3].wait()
        at = pl.ds(pl.multiple_of(dat * cap_dev, cap_dev), cap_dev)
        for e in range(experts_dev):
            score = jnp.zeros((cap_dev, LANES), f32)
            for b in range(PAIR * chunks):
                weight = router_ref[e : e + 1, b * LANES : (b + 1) * LANES].astype(f32)
                score += rows[b, e, at].astype(f32) * weight
            gate[e] = jax.nn.sigmoid(jnp.sum(score, axis=-1, keepdims=True))

    def stage_weigh(k, p):
        back_y(k, p).wait_recv()
        summed = kept[k, pair(p)] + y_recv[k, pair(p)].astype(f32)
        own, other = split(gate[pair(p)] * summed)
        give[k, pair(p)] = other.astype(bf16)
        ref = raw.at[k, 1, pair(p)]
        send(copy_to(give.at[k, pair(p)], ref, 13, raw_sem, (k,), near_diag), is_end)
        send(back_x(k, p))
        slots_v[k, 0, pair(p)] = own.astype(bf16)
        send(raw_copy(k, 0, p), is_end)

    def stage_cross(k, p):
        back_x(k, p).wait_recv()

    def dest_out(k, j, total, peer, peer_diag):
        for xr in (1, 0):
            dest_send[k, j, xr] = total[xr * tok_rows : (xr + 1) * tok_rows].astype(bf16)
            dest_copy(k, j, xr, peer_diag if k == last and xr == 1 else peer).start()

    def last_out(k, total):
        last_send[k] = total.astype(bf16)
        last_copy(k).start()

    def stage_place(k):
        held = slots_v[k].reshape(PAIR * slots, LANES)

        @pl.when(is_inner)
        def _():
            dest_out(k, 0, jnp.dot(place_own[:both, :], held, preferred_element_type=f32), near, near_diag)

        at = pl.ds(pl.multiple_of(spot * both, both), both)
        total = jnp.dot(place_own[at, :], held, preferred_element_type=f32)
        dense[k] = total
        if k == last:

            @pl.when(is_end)
            def _():
                last_out(k, total[tok_rows:])

    def stage_far(k):
        @pl.when(is_inner)
        def _():
            held = slots_v[k].reshape(PAIR * slots, LANES)
            mine = jnp.dot(place_own[2 * both :, :], held, preferred_element_type=f32)
            copy_to(raw.at[k], raw.at[k], 13, raw_sem, (k,), near).wait_recv()
            ends = raw[k].reshape(PAIR * slots, LANES)
            theirs = jnp.dot(place_far[2 * both :, :], ends, preferred_element_type=f32)
            dest_out(k, 2, mine[both:] + theirs, far_end, far_end_diag)
            theirs = jnp.dot(place_far[both : 2 * both, :], ends, preferred_element_type=f32)
            dest_out(k, 1, mine[:both] + theirs, far_inner, far_diag)
            total = dense[k] + jnp.dot(place_far[:both, :], ends, preferred_element_type=f32)
            dense[k] = total
            if k == last:
                last_out(k, total[tok_rows:])

    def arrived(k, xr, ref):
        copy_to(ref, ref, 14, dest_sem, (k, xr), near).wait_recv()

    def stage_total(k):
        def finish(total, xr):
            if xr == 1:
                last_out(k, total)
            else:
                last_own[k] = total

        where = (0,) if k == last else (1, 0)

        @pl.when(is_end)
        def _():
            for xr in where:
                arrived(k, xr, dest_recv.at[k, :, xr])
                held = dense[k, xr * tok_rows : (xr + 1) * tok_rows]
                finish(held + dest_recv[k, 0, xr].astype(f32) + dest_recv[k, 1, xr].astype(f32), xr)

        @pl.when(is_inner)
        def _():
            for xr in where:
                arrived(k, xr, dest_recv.at[k, 1, xr])
                held = dense[k, xr * tok_rows : (xr + 1) * tok_rows]
                finish(held + dest_recv[k, 1, xr].astype(f32), xr)

    def stage_last(k):
        def finish(own, other):
            cols = slice(k * wide, (k + 1) * wide)
            left, right = jnp.where(x == 0, own, other), jnp.where(x == 0, other, own)
            total = jnp.concatenate([left, right], axis=1)
            out_ref[:, cols] = (tokens_ref[:, cols].astype(f32) + total).astype(bf16)

        last_copy(k).wait_recv()
        own, other = last_own[k], last_recv[k].astype(f32)
        if k < last:
            finish(own, other)
            return

        @pl.when(is_end)
        def _():
            arrived(k, 1, dest_recv.at[k, :, 1])
            finish(own, other + dest_recv[k, 0, 1].astype(f32) + dest_recv[k, 1, 1].astype(f32))

        @pl.when(is_inner)
        def _():
            arrived(k, 1, dest_recv.at[k, 1, 1])
            finish(own, other + dest_recv[k, 1, 1].astype(f32))

    def run_first(k):
        for p in range(PARTS):
            stage_first(k, p)
            if k == last:
                stage_second(0, p)

    order = [(-6.0, stage_ids, ())]
    for k in range(chunks):
        order += [
            (CROSS_IN[k], stage_cross_in, (k,)),
            (2.8 * k - 2.65, stage_far_pick, (k,)),
            (2.8 * k, stage_pick, (k,)),
            (2.8 * k + 3.1, stage_swap, (k,)),
            (2.8 * k + 3.9, stage_relay, (k, 0)),
            (RELAY_AT[k], stage_relay, (k, 1)),
            (FIRST_AT[k], run_first, (k,)),
        ]
    for _, stage, where in sorted(order, key=lambda step: step[0]):
        stage(*where)

    pieces = [(k, p) for k in range(chunks) for p in range(PARTS)]
    for i in range(PARTS, len(pieces)):
        stage_second(*pieces[i])
        stage_core(*pieces[i - PARTS])
    gates()
    for i in range(len(pieces) - PARTS, len(pieces)):
        stage_core(*pieces[i])

    order = []
    for k in range(chunks):
        order += [
            (2 * k + 0.0, stage_weigh, (k, 0)),
            (2 * k + 1.0, stage_weigh, (k, 1)),
            (2 * k + 2.1, stage_cross, (k, 0)),
            (2 * k + 3.1, stage_cross, (k, 1)),
            (2 * k + 3.2, stage_place, (k,)),
            (2 * k + 6.05, stage_far, (k,)),
            (2 * k + 11.4, stage_total, (k,)),
            (2 * k + 15.6, stage_last, (k,)),
        ]
    for _, stage, where in sorted(order, key=lambda step: step[0]):
        stage(*where)

    def sent(ref, stage, cond=None):
        done = copy_to(ref, ref, stage, ids_sem, (0,), x_peer)
        if cond is None:
            done.wait_send()
        else:
            pl.when(cond)(done.wait_send)

    own_all = rows.at[:, :, dat_at(dat)]
    sent(cross, 0)
    sent(ids_ref, 1)
    sent(ids_all.at[2:4], 2, is_end)
    sent(blocks.at[0], 3, is_end)
    sent(blocks.at[0], 4)
    sent(pick_send, 5, is_inner)
    sent(swap_send, 6)
    for stage in (7, 8, 9):
        sent(own_all, stage)
    sent(parts.at[:, :, 1 - c], 10)
    sent(y_send, 11)
    sent(give, 12)
    sent(slots_v, 13, is_end)
    sent(dest_send, 14, is_inner)
    sent(last_send, 15)


def kernel_body(tokens, norm_gain, router_weight, inner_weight, outer_weight, slot_tokens, slot_ids):
    del slot_ids
    tok_rows, width = tokens.shape
    experts_dev, cap_dev = slot_tokens.shape
    units = inner_weight.shape[2]
    dat_count = lax.axis_size("dat")
    slots = experts_dev * cap_dev
    wide = PAIR * LANES
    chunks = width // wide
    both = PAIR * tok_rows
    bf16, f32 = jnp.bfloat16, jnp.float32
    vmem = pl.BlockSpec(memory_space=pltpu.VMEM)
    hbm = pl.BlockSpec(memory_space=pltpu.HBM)
    dma = pltpu.SemaphoreType.DMA

    def buffer(*shape, kind=bf16):
        return pltpu.VMEM(shape, kind)

    return pl.pallas_call(
        moe_kernel,
        out_shape=jax.ShapeDtypeStruct((tok_rows, width), bf16),
        in_specs=[hbm] * 6,
        out_specs=vmem,
        scratch_shapes=[
            buffer(tok_rows, width),
            buffer(1, width, kind=f32),
            buffer(experts_dev, width),
            buffer(experts_dev, cap_dev, kind=jnp.int32),
            buffer(experts_dev, width, units),
            buffer(experts_dev, units, width),
            buffer(LINE, experts_dev, cap_dev, kind=jnp.int32),
            buffer(PAIR * slots, LINE * both),
            buffer(LINE * both, PAIR * slots),
            buffer(PAIR * slots, (LINE - 1) * both),
            buffer((LINE - 1) * both, PAIR * slots),
            buffer(chunks, LINE, PAIR, tok_rows, LANES),
            buffer(chunks, tok_rows, LANES),
            buffer(chunks, PAIR, experts_dev, cap_dev, LANES),
            buffer(chunks, PAIR, experts_dev, cap_dev, LANES),
            buffer(chunks, experts_dev, cap_dev, LANES),
            buffer(PAIR * chunks, experts_dev, dat_count * cap_dev, LANES),
            buffer(experts_dev, dat_count * cap_dev, units, kind=f32),
            buffer(experts_dev, dat_count * cap_dev, units),
            buffer(experts_dev, cap_dev, 1, kind=f32),
            buffer(chunks, PAIR, PAIR, experts_dev, cap_dev, wide),
            buffer(chunks, PAIR, experts_dev, cap_dev, wide),
            buffer(chunks, experts_dev, cap_dev, wide),
            buffer(chunks, experts_dev, cap_dev, wide),
            buffer(chunks, experts_dev, cap_dev, wide, kind=f32),
            buffer(chunks, experts_dev, cap_dev, LANES),
            buffer(chunks, PAIR, experts_dev, cap_dev, LANES),
            buffer(chunks, PAIR, experts_dev, cap_dev, LANES),
            buffer(chunks, both, LANES, kind=f32),
            buffer(chunks, LINE - 1, PAIR, tok_rows, LANES),
            buffer(chunks, 2, PAIR, tok_rows, LANES),
            buffer(chunks, tok_rows, LANES),
            buffer(chunks, tok_rows, LANES),
            buffer(chunks, tok_rows, LANES, kind=f32),
            dma((6,)),
            dma((16,)),
            dma((2,)),
            dma((chunks,)),
            dma((chunks,)),
            dma((chunks,)),
            dma((chunks, PAIR, PARTS)),
            dma((chunks, PARTS)),
            dma((chunks, PAIR, PARTS)),
            dma((chunks, PARTS)),
            dma((chunks, PARTS)),
            dma((chunks, PARTS)),
            dma((chunks, PARTS)),
            dma((chunks, PARTS)),
            dma((chunks,)),
            dma((chunks, PAIR)),
            dma((chunks,)),
        ],
        compiler_params=pltpu.CompilerParams(
            collective_id=0, has_side_effects=True, vmem_limit_bytes=48 * 1024 * 1024
        ),
    )(
        *(
            pltpu.with_memory_space_constraint(array, pltpu.HBM)
            for array in (tokens, norm_gain.reshape(1, width), router_weight.T, slot_tokens)
        ),
        inner_weight,
        outer_weight,
    )


def solution(mesh):
    fits = mesh.shape["dat"] == PAIR * PAIR and mesh.shape["exp"] == PAIR * LINE
    chosen = kernel_body if fits else body
    in_specs = (
        P(("exp", "dat"), None),
        P(),
        P(None, "exp"),
        P("exp", None, "dat"),
        P("exp", "dat", None),
        P("exp", "dat"),
        P(("exp", "dat"), None),
    )
    out_specs = P(("exp", "dat"), None)
    return jax.shard_map(chosen, mesh=mesh, in_specs=in_specs, out_specs=out_specs, check_vma=False)
```

```python
import jax
import jax.numpy as jnp
from jax import lax
from jax.experimental import pallas as pl
from jax.experimental.pallas import tpu as pltpu
from jax.sharding import PartitionSpec as P

EPSILON = 1e-06


def normalize(tokens, norm_gain):
    values = tokens.astype(jnp.float32)
    scale = lax.rsqrt(jnp.mean(values * values, axis=-1, keepdims=True) + EPSILON)
    return (values * scale * norm_gain).astype(jnp.bfloat16)


def owner_places(slot_ids, experts_dev, capacity, bucket):
    flat_ids = slot_ids.reshape(-1)
    source = flat_ids // capacity // experts_dev
    before = (source[:, None] == source[None, :]) & (flat_ids[None, :] < flat_ids[:, None])
    ranks_in = jnp.sum(before.astype(jnp.int32), axis=1)
    return (source * bucket + ranks_in).reshape(slot_ids.shape)


def expert_places(token_ids, slot_keys, tok_rows, dat_count, bucket):
    owner_of = token_ids // (tok_rows * dat_count)
    before = (owner_of[:, None] == owner_of[None, :]) & (slot_keys[None, :] < slot_keys[:, None])
    ranks_in = jnp.sum(before.astype(jnp.int32), axis=1)
    return owner_of * bucket + ranks_in


def body(tokens, norm_gain, router_weight, inner_weight, outer_weight, slot_tokens, slot_ids):
    exp_count = lax.axis_size("exp")
    dat_count = lax.axis_size("dat")
    tok_rows, width = tokens.shape
    experts_dev, cap_dev = slot_tokens.shape
    bucket = 6 * tok_rows // exp_count
    normed = normalize(tokens, norm_gain)
    picked = slot_tokens.T.reshape(-1)
    expert_iota = lax.broadcasted_iota(jnp.int32, (cap_dev, experts_dev), 1)
    column_iota = lax.broadcasted_iota(jnp.int32, (cap_dev, experts_dev), 0)
    slot_keys = (expert_iota * cap_dev + column_iota).reshape(-1)
    senders = expert_places(picked, slot_keys, tok_rows, dat_count, bucket)
    receivers = owner_places(slot_ids, experts_dev, cap_dev * dat_count, bucket)
    lookup = jnp.any(
        lax.broadcasted_iota(jnp.int32, (exp_count * bucket, 1, 1), 0) == receivers[None], axis=2
    )
    outgoing = jnp.dot(lookup.astype(jnp.bfloat16), normed, preferred_element_type=jnp.float32)
    outgoing = outgoing.astype(jnp.bfloat16).reshape(exp_count, bucket, width)
    arrived = lax.all_to_all(outgoing, "exp", split_axis=0, concat_axis=0, tiled=True).reshape(
        exp_count * bucket, width
    )
    gathered_rows = jnp.take(arrived, senders, axis=0)
    gathered_rows = gathered_rows.reshape(cap_dev, experts_dev, width)
    gate_score = jax.nn.sigmoid(
        jnp.einsum("ced,de->ce", gathered_rows, router_weight, preferred_element_type=jnp.float32)
    )
    inner = jnp.einsum(
        "ced,edf->cef",
        lax.all_gather(gathered_rows, "dat", axis=0, tiled=True),
        inner_weight,
        preferred_element_type=jnp.float32,
    )
    hidden = jax.nn.relu(inner).astype(jnp.bfloat16)
    expert_out = lax.psum_scatter(
        jnp.einsum("cef,efd->ced", hidden, outer_weight, preferred_element_type=jnp.float32).astype(
            jnp.bfloat16
        ),
        "dat",
        scatter_dimension=0,
        tiled=True,
    ).astype(jnp.float32)
    weighted = (gate_score[:, :, None] * expert_out).astype(jnp.bfloat16).reshape(-1, width)
    placing = lax.broadcasted_iota(jnp.int32, (exp_count * bucket, 1), 0) == senders[None, :]
    returning = jnp.dot(placing.astype(jnp.bfloat16), weighted, preferred_element_type=jnp.float32)
    returning = returning.astype(jnp.bfloat16).reshape(exp_count, bucket, width)
    came_back = lax.all_to_all(returning, "exp", split_axis=0, concat_axis=0, tiled=True).reshape(
        exp_count * bucket, width
    )
    combine_table = jnp.sum(
        (
            lax.broadcasted_iota(jnp.int32, (1, 1, exp_count * bucket), 2) == receivers[:, :, None]
        ).astype(jnp.float32),
        axis=1,
    )
    combined = jnp.dot(
        combine_table.astype(jnp.bfloat16), came_back, preferred_element_type=jnp.float32
    )
    return (tokens.astype(jnp.float32) + combined).astype(jnp.bfloat16)


MESH = pl.DeviceIdType.MESH
PAIR = 2
LINE = 4
LANES = 128
PARTS = 2
SENT_BY = {1: 1, 2: 2, 3: 3, 13: 3, 5: 4, 14: 4}
FIRST_AT = (9.6, 11.3, 14.5, 16.8)
RELAY_AT = (5.65, 8.45, 11.25, 12.4)
CROSS_IN = (-5.5, -5.4, -2.6, -1.9)


def moe_kernel(
    tokens_hbm, gain_hbm, router_hbm, ids_hbm, inner_hbm, outer_hbm, out_ref,
    tokens_ref, gain_ref, router_ref, ids_ref, inner_v, outer_v, ids_all, pick_own, place_own, pick_far, place_far,
    blocks, cross, pick_send, pick_recv, swap_send, rows, sums, hidden, gate,
    parts, core_recv, y_send, y_recv, kept, give, slots_v, raw, dense, dest_send, dest_recv,
    last_send, last_recv, last_own,
    w_sem, out_sem, ids_sem, x_sem, near_sem, far_sem, pick_sem, swap_sem, y_sem, c_sem, cr_sem,
    rc_sem, ry_sem, rx_sem, raw_sem, dest_sem, last_sem,
):
    chunks = blocks.shape[0]
    tok_rows = tokens_ref.shape[0]
    experts_dev, cap_dev = ids_ref.shape
    slots = experts_dev * cap_dev
    both = PAIR * tok_rows
    wide = PAIR * LANES
    pair_e = experts_dev // PARTS
    bf16, f32 = jnp.bfloat16, jnp.float32
    exp = lax.axis_index("exp")
    dat = lax.axis_index("dat")
    dat_count = lax.axis_size("dat")
    z, x = exp // PAIR, exp % PAIR
    y, c = dat // PAIR, dat % PAIR
    half = z // PAIR
    spot = z + half * (LINE - 1 - 2 * z)
    is_end = spot == 0
    is_inner = spot == 1

    def line_z(q):
        return q + half * (LINE - 1 - 2 * q)

    near = (line_z(1 - spot) * PAIR + x, dat)
    far_inner = (line_z(2) * PAIR + x, dat)
    far_end = (line_z(3) * PAIR + x, dat)
    x_peer = (exp + 1 - 2 * x, dat)
    y_peer = (exp, dat + PAIR - 2 * PAIR * y)
    c_peer = (exp, dat + 1 - 2 * c)
    near_diag = (line_z(1 - spot) * PAIR + 1 - x, dat)
    far_diag = (line_z(2) * PAIR + 1 - x, dat)
    far_end_diag = (line_z(3) * PAIR + 1 - x, dat)
    xy_diag = (exp + 1 - 2 * x, dat + PAIR - 2 * PAIR * y)
    last = chunks - 1

    def copy_to(src, dst, stage, sems, where, peer):
        return pltpu.make_async_remote_copy(
            src_ref=src, dst_ref=dst, send_sem=out_sem.at[SENT_BY.get(stage, 0)],
            recv_sem=sems.at[where], device_id=peer, device_id_type=MESH,
        )

    def send(copy, cond=None):
        if cond is None:
            copy.start()
        else:
            pl.when(cond)(copy.start)

    loads = []
    for e in range(experts_dev):
        loads.append(pltpu.make_async_copy(inner_hbm.at[e], inner_v.at[e], w_sem.at[0]))
    for e in range(experts_dev):
        loads.append(pltpu.make_async_copy(outer_hbm.at[e], outer_v.at[e], w_sem.at[1]))
    inner_load = pltpu.make_async_copy(inner_hbm, inner_v, w_sem.at[0])
    outer_load = pltpu.make_async_copy(outer_hbm, outer_v, w_sem.at[1])

    barrier = pltpu.get_barrier_semaphore()
    for peer in (near, near_diag, far_inner, far_diag, x_peer, y_peer, xy_diag, c_peer):
        pl.semaphore_signal(barrier, inc=1, device_id=peer, device_id_type=MESH)

    @pl.when(is_inner)
    def _():
        for peer in (far_end, far_end_diag):
            pl.semaphore_signal(barrier, inc=1, device_id=peer, device_id_type=MESH)

    smalls = []
    for i, (src, dst) in enumerate(
        ((ids_hbm, ids_ref), (tokens_hbm, tokens_ref), (gain_hbm, gain_ref), (router_hbm, router_ref))
    ):
        smalls.append(pltpu.make_async_copy(src, dst, w_sem.at[2 + i]))
        smalls[i].start()
    for load in loads:
        load.start()
    smalls[1].wait()
    smalls[2].wait()

    values = tokens_ref[...].astype(f32)
    scale = lax.rsqrt(jnp.mean(values * values, axis=-1, keepdims=True) + EPSILON)
    normed = values * scale * gain_ref[...]

    def split(value):
        low, high = value[..., :LANES], value[..., LANES:]
        return jnp.where(x == 0, low, high), jnp.where(x == 0, high, low)

    for k in range(chunks):
        own, other = split(normed[:, k * wide : (k + 1) * wide])
        blocks[k, spot, 0] = own.astype(bf16)
        cross[k] = other.astype(bf16)

    def one_hots(ids, side, pick, place, first):
        row = jnp.concatenate([ids[e : e + 1, :] for e in range(experts_dev)], axis=1)
        column = jnp.broadcast_to(row, (LANES, slots)).T
        lane = lax.broadcasted_iota(jnp.int32, (slots, tok_rows), 1)
        line = lax.broadcasted_iota(jnp.int32, (tok_rows, slots), 0)
        at = slice(side * slots, (side + 1) * slots)
        for q in range(first, LINE):
            for xr in range(PAIR):
                x_of = x if xr == 0 else 1 - x
                base = ((line_z(q) * PAIR + x_of) * dat_count + dat) * tok_rows
                start = ((q - first) * PAIR + xr) * tok_rows
                span = slice(start, start + tok_rows)
                pick[at, span] = (column == lane + base).astype(f32).astype(bf16)
                place[span, at] = (row == line + base).astype(f32).astype(bf16)

    smalls[0].wait()

    pl.semaphore_wait(barrier, 8 + 2 * is_inner.astype(jnp.int32))

    def cross_copy(k):
        return copy_to(cross.at[k], blocks.at[k, spot, 1], 0, x_sem, (k,), x_peer)

    ids_x = copy_to(ids_ref, ids_all.at[1], 1, ids_sem, (0,), x_peer)
    ids_near = copy_to(ids_ref, ids_all.at[2], 2, ids_sem, (1,), near)
    ids_diag = copy_to(ids_ref, ids_all.at[3], 2, ids_sem, (1,), near_diag)
    ids_both = copy_to(ids_all.at[2:4], ids_all.at[2:4], 2, ids_sem, (1,), near)

    def near_copy(k, xr):
        ref = blocks.at[k, 0, xr]
        return copy_to(ref, ref, 3, near_sem, (k,), near)

    def far_copy(k, xr):
        return copy_to(blocks.at[k, spot, xr], blocks.at[k, 3 - spot, xr], 4, far_sem, (k,), far_inner)

    def block_send(k, xr):
        send(far_copy(k, xr))
        send(near_copy(k, xr), is_end)

    def diag_send(k):
        send(copy_to(cross.at[k], blocks.at[k, 3 - spot, 1], 4, far_sem, (k,), far_diag))
        send(copy_to(cross.at[k], blocks.at[k, 0, 1], 3, near_sem, (k,), near_diag), is_end)

    send(ids_x)
    send(ids_near, is_end)
    send(ids_diag, is_end)
    send(cross_copy(0))
    diag_send(0)
    block_send(0, 0)
    send(cross_copy(1))
    block_send(1, 0)
    block_send(2, 0)
    for k in range(2, chunks):
        send(cross_copy(k))

    def stage_cross_in(k):
        cross_copy(k).wait_recv()
        if k > 0:
            block_send(k, 1)
        if k == 1:
            for j in range(3, chunks):
                block_send(j, 0)

    def stage_ids():
        one_hots(ids_ref, 0, pick_own, place_own, 0)
        ids_x.wait_recv()
        one_hots(ids_all.at[1], 1, pick_own, place_own, 0)

        @pl.when(is_inner)
        def _():
            ids_both.wait_recv()
            one_hots(ids_all.at[2], 0, pick_far, place_far, 1)
            one_hots(ids_all.at[3], 1, pick_far, place_far, 1)

    def pair(p):
        return slice(p * pair_e, (p + 1) * pair_e)

    def own_rows(k, rel, p, of_dat):
        feature = k * PAIR + (x if rel == 0 else 1 - x)
        at = pl.ds(pl.multiple_of(of_dat * cap_dev, cap_dev), cap_dev)
        return rows.at[feature, pair(p), at]

    def late_at(k, p):
        return (k + p if k == last else k,)

    def dat_at(of_dat):
        return pl.ds(pl.multiple_of(of_dat * cap_dev, cap_dev), cap_dev)

    def pick_copy(k, xr, p):
        return copy_to(
            pick_send.at[k, xr, pair(p)], pick_recv.at[k, xr, pair(p)], 5, pick_sem, (k, xr, p), near
        )

    def swap_copy(k, p):
        return copy_to(
            swap_send.at[k, pair(p)], own_rows(k, 0, p, dat), 6, swap_sem, (k, p), x_peer
        )

    def far_swap(k, p):
        return copy_to(
            swap_send.at[k, pair(p)], own_rows(k, 0, p, dat), 7, y_sem, (k, 1, p), xy_diag
        )

    def y_copy(k, rel, p, of_dat):
        ref = own_rows(k, rel, p, of_dat)
        return copy_to(ref, ref, 7, y_sem, (k, rel, p), y_peer)

    def c_copy(k, rel, p, of_dat):
        ref = own_rows(k, rel, p, of_dat)
        return copy_to(ref, ref, 8, c_sem, late_at(k, p), c_peer)

    def relay_copy(k, rel, p, of_dat):
        ref = own_rows(k, rel, p, of_dat)
        return copy_to(ref, ref, 9, cr_sem, late_at(k, p), c_peer)

    def both_rows(k, p, of_dat):
        parts_at = pair(p) if k == last else slice(0, experts_dev)
        return rows.at[k * PAIR : (k + 1) * PAIR, parts_at, dat_at(of_dat)]

    dat_y = dat + PAIR - 2 * PAIR * y
    dat_c = dat + 1 - 2 * c
    dat_yc = dat_y + 1 - 2 * c

    def by_part(value):
        size = pair_e * cap_dev
        return [
            value[p * size : (p + 1) * size].reshape(pair_e, cap_dev, LANES) for p in range(PARTS)
        ]

    def sides(k):
        return (1, 0) if k + 1 == chunks else (0, 1)

    def stage_far_pick(k):
        @pl.when(is_inner)
        def _():
            near_all, far_all = blocks.at[k, 0], blocks.at[k, 2:4]
            copy_to(near_all, near_all, 3, near_sem, (k,), near).wait_recv()
            copy_to(far_all, far_all, 4, far_sem, (k,), far_inner).wait_recv()
            found = blocks[k].reshape(LINE * both, LANES)
            for xr in sides(k):
                at = slice(xr * slots, (xr + 1) * slots)
                got = jnp.dot(pick_far[at, :], found[both:], preferred_element_type=f32)
                got = by_part(got.astype(bf16))
                for p in range(PARTS):
                    pick_send[k, xr, pair(p)] = got[p]
                    pick_copy(k, xr, p).start()

    def hand_on(k, xr, p, value):
        if xr == 1:
            swap_send[k, pair(p)] = value
            swap_copy(k, p).start()
            far_swap(k, p).start()
        else:
            own_rows(k, 0, p, dat)[...] = value
            y_copy(k, 0, p, dat).start()
            c_copy(k, 0, p, dat).start()

    def stage_pick(k):
        @pl.when(is_inner)
        def _():
            found = blocks[k].reshape(LINE * both, LANES)
            for xr in (1, 0):
                at = slice(xr * slots, (xr + 1) * slots)
                got = jnp.dot(pick_own[at, :], found, preferred_element_type=f32)
                got = by_part(got.astype(bf16))
                for p in range(PARTS):
                    hand_on(k, xr, p, got[p])

        @pl.when(is_end)
        def _():
            found = blocks[k, 0].reshape(both, LANES)
            for xr in sides(k):
                at = slice(xr * slots, (xr + 1) * slots)
                got = by_part(jnp.dot(pick_own[at, :both], found, preferred_element_type=f32))
                for p in range(PARTS):
                    pick_copy(k, xr, p).wait_recv()
                    here = got[p] + pick_recv[k, xr, pair(p)].astype(f32)
                    hand_on(k, xr, p, here.astype(bf16))

    def stage_swap(k):
        for p in range(PARTS):
            ref = own_rows(k, 1, p, dat)
            copy_to(ref, ref, 6, swap_sem, (k, p), x_peer).wait_recv()
            send(c_copy(k, 1, p, dat))

    def stage_relay(k, rel):
        for p in range(PARTS):
            y_copy(k, rel, p, dat_y).wait_recv()
            send(relay_copy(k, rel, p, dat_y))

    def stage_first(k, p):
        for sems, stage, of_dat in ((c_sem, 8, dat_c), (cr_sem, 9, dat_yc)):
            if k == last or p == 0:
                ref = both_rows(k, p, of_dat)
                copy_to(ref, ref, stage, sems, late_at(k, p), c_peer).wait_recv()
        if k == 0 and p == 0:
            inner_load.wait()

        for e in range(p * pair_e, (p + 1) * pair_e):
            left = jnp.concatenate([rows[PAIR * k, e], rows[PAIR * k + 1, e]], axis=1)
            total = jnp.dot(left, inner_v[e, k * wide : (k + 1) * wide, :], preferred_element_type=f32)
            if k > 0:
                total += sums[e]
            if k + 1 < chunks:
                sums[e] = total
            else:
                hidden[e] = jnp.maximum(total, 0.0).astype(bf16)

    def core_copy(k, p):
        return copy_to(
            parts.at[k, :, 1 - c, pair(p)], core_recv.at[k, :, pair(p)], 10, rc_sem, (k, p), c_peer
        )

    def back_y(k, p):
        return copy_to(y_send.at[k, pair(p)], y_recv.at[k, pair(p)], 11, ry_sem, (k, p), y_peer)

    def back_x(k, p):
        return copy_to(give.at[k, pair(p)], slots_v.at[k, 1, pair(p)], 12, rx_sem, (k,), x_peer)

    def raw_copy(k, xr, p):
        return copy_to(
            slots_v.at[k, xr, pair(p)], raw.at[k, xr, pair(p)], 13, raw_sem, (k,), near
        )

    def dest_copy(k, j, xr, peer):
        return copy_to(
            dest_send.at[k, j, xr], dest_recv.at[k, min(j, 1), xr], 14, dest_sem, (k, xr), peer
        )

    def last_copy(k):
        return copy_to(last_send.at[k], last_recv.at[k], 15, last_sem, (k,), x_peer)

    def stage_second(k, p):
        if k == 0 and p == 0:
            outer_load.wait()
        for e in range(p * pair_e, (p + 1) * pair_e):
            part = jnp.dot(
                hidden[e], outer_v[e, :, k * wide : (k + 1) * wide], preferred_element_type=f32
            ).astype(bf16)
            for d in range(PAIR * PAIR):
                parts[k, d // PAIR, d % PAIR, e] = part[d * cap_dev : (d + 1) * cap_dev]
        send(core_copy(k, p))

    def stage_core(k, p):
        core_copy(k, p).wait_recv()
        theirs = parts[k, 1 - y, c, pair(p)].astype(f32) + core_recv[k, 1 - y, pair(p)].astype(f32)
        y_send[k, pair(p)] = theirs.astype(bf16)
        send(back_y(k, p))
        ours = parts[k, y, c, pair(p)].astype(f32) + core_recv[k, y, pair(p)].astype(f32)
        kept[k, pair(p)] = ours

    def gates():
        smalls[3].wait()
        at = pl.ds(pl.multiple_of(dat * cap_dev, cap_dev), cap_dev)
        for e in range(experts_dev):
            score = jnp.zeros((cap_dev, LANES), f32)
            for b in range(PAIR * chunks):
                weight = router_ref[e : e + 1, b * LANES : (b + 1) * LANES].astype(f32)
                score += rows[b, e, at].astype(f32) * weight
            gate[e] = jax.nn.sigmoid(jnp.sum(score, axis=-1, keepdims=True))

    def stage_weigh(k, p):
        back_y(k, p).wait_recv()
        summed = kept[k, pair(p)] + y_recv[k, pair(p)].astype(f32)
        own, other = split(gate[pair(p)] * summed)
        give[k, pair(p)] = other.astype(bf16)
        ref = raw.at[k, 1, pair(p)]
        send(copy_to(give.at[k, pair(p)], ref, 13, raw_sem, (k,), near_diag), is_end)
        send(back_x(k, p))
        slots_v[k, 0, pair(p)] = own.astype(bf16)
        send(raw_copy(k, 0, p), is_end)

    def stage_cross(k):
        ref = slots_v.at[k, 1]
        copy_to(ref, ref, 12, rx_sem, (k,), x_peer).wait_recv()

    def dest_out(k, j, total, peer, peer_diag):
        for xr in (1, 0):
            dest_send[k, j, xr] = total[xr * tok_rows : (xr + 1) * tok_rows].astype(bf16)
            dest_copy(k, j, xr, peer_diag if k == last and xr == 1 else peer).start()

    def last_out(k, total):
        last_send[k] = total.astype(bf16)
        last_copy(k).start()

    def stage_place(k):
        held = slots_v[k].reshape(PAIR * slots, LANES)

        @pl.when(is_inner)
        def _():
            dest_out(k, 0, jnp.dot(place_own[:both, :], held, preferred_element_type=f32), near, near_diag)

        at = pl.ds(pl.multiple_of(spot * both, both), both)
        total = jnp.dot(place_own[at, :], held, preferred_element_type=f32)
        dense[k] = total
        if k == last:

            @pl.when(is_end)
            def _():
                last_out(k, total[tok_rows:])

    def stage_far(k):
        @pl.when(is_inner)
        def _():
            held = slots_v[k].reshape(PAIR * slots, LANES)
            mine = jnp.dot(place_own[2 * both :, :], held, preferred_element_type=f32)
            copy_to(raw.at[k], raw.at[k], 13, raw_sem, (k,), near).wait_recv()
            ends = raw[k].reshape(PAIR * slots, LANES)
            theirs = jnp.dot(place_far[2 * both :, :], ends, preferred_element_type=f32)
            dest_out(k, 2, mine[both:] + theirs, far_end, far_end_diag)
            theirs = jnp.dot(place_far[both : 2 * both, :], ends, preferred_element_type=f32)
            dest_out(k, 1, mine[:both] + theirs, far_inner, far_diag)
            total = dense[k] + jnp.dot(place_far[:both, :], ends, preferred_element_type=f32)
            dense[k] = total
            if k == last:
                last_out(k, total[tok_rows:])

    def arrived(k, xr, ref):
        copy_to(ref, ref, 14, dest_sem, (k, xr), near).wait_recv()

    def stage_total(k):
        def finish(total, xr):
            if xr == 1:
                last_out(k, total)
            else:
                last_own[k] = total

        where = (0,) if k == last else (1, 0)

        @pl.when(is_end)
        def _():
            for xr in where:
                arrived(k, xr, dest_recv.at[k, :, xr])
                held = dense[k, xr * tok_rows : (xr + 1) * tok_rows]
                finish(held + dest_recv[k, 0, xr].astype(f32) + dest_recv[k, 1, xr].astype(f32), xr)

        @pl.when(is_inner)
        def _():
            for xr in where:
                arrived(k, xr, dest_recv.at[k, 1, xr])
                held = dense[k, xr * tok_rows : (xr + 1) * tok_rows]
                finish(held + dest_recv[k, 1, xr].astype(f32), xr)

    def stage_last(k):
        def finish(own, other):
            cols = slice(k * wide, (k + 1) * wide)
            left, right = jnp.where(x == 0, own, other), jnp.where(x == 0, other, own)
            total = jnp.concatenate([left, right], axis=1)
            out_ref[:, cols] = (tokens_ref[:, cols].astype(f32) + total).astype(bf16)

        last_copy(k).wait_recv()
        own, other = last_own[k], last_recv[k].astype(f32)
        if k < last:
            finish(own, other)
            return

        @pl.when(is_end)
        def _():
            arrived(k, 1, dest_recv.at[k, :, 1])
            finish(own, other + dest_recv[k, 0, 1].astype(f32) + dest_recv[k, 1, 1].astype(f32))

        @pl.when(is_inner)
        def _():
            arrived(k, 1, dest_recv.at[k, 1, 1])
            finish(own, other + dest_recv[k, 1, 1].astype(f32))

    def run_first(k):
        for p in range(PARTS):
            stage_first(k, p)
            if k == last:
                stage_second(0, p)

    order = [(-6.0, stage_ids, ())]
    for k in range(chunks):
        order += [
            (CROSS_IN[k], stage_cross_in, (k,)),
            (2.8 * k - 2.65, stage_far_pick, (k,)),
            (2.8 * k, stage_pick, (k,)),
            (2.8 * k + 3.1, stage_swap, (k,)),
            (2.8 * k + 3.9, stage_relay, (k, 0)),
            (RELAY_AT[k], stage_relay, (k, 1)),
            (FIRST_AT[k], run_first, (k,)),
        ]
    for _, stage, where in sorted(order, key=lambda step: step[0]):
        stage(*where)

    pieces = [(k, p) for k in range(chunks) for p in range(PARTS)]
    for i in range(PARTS, len(pieces)):
        stage_second(*pieces[i])
        stage_core(*pieces[i - PARTS])
    gates()
    for i in range(len(pieces) - PARTS, len(pieces)):
        stage_core(*pieces[i])

    order = []
    for k in range(chunks):
        order += [
            (2 * k + 0.0, stage_weigh, (k, 0)),
            (2 * k + 1.0, stage_weigh, (k, 1)),
            (2 * k + 3.1, stage_cross, (k,)),
            (2 * k + 3.2, stage_place, (k,)),
            (2 * k + 6.05, stage_far, (k,)),
            (2 * k + 11.4, stage_total, (k,)),
            (2 * k + 15.6, stage_last, (k,)),
        ]
    for _, stage, where in sorted(order, key=lambda step: step[0]):
        stage(*where)

    def count(*refs):
        total = 0
        for ref in refs:
            size = 1
            for extent in ref.shape:
                size *= extent
            total += size
        return total

    def sent(ref, stage, cond=None):
        done = copy_to(ref, ref, stage, ids_sem, (0,), x_peer)
        if cond is None:
            done.wait_send()
        else:
            pl.when(cond)(done.wait_send)

    width, units = inner_v.shape[1], inner_v.shape[2]

    def sized(total):
        whole_e, lines = divmod(total, width * units)
        if lines == 0:
            return outer_v.at[0:whole_e]
        assert whole_e == 0 and lines % width == 0
        return outer_v.at[0, 0 : lines // width]

    own_all = rows.at[:, :, dat_at(dat)]
    half_parts = parts.at[:, :, 1 - c]
    always = count(cross, blocks.at[0], swap_send, own_all, own_all, own_all, half_parts)
    always += count(y_send, give, last_send)
    sent(sized(always), 0)
    sent(ids_ref, 1)
    sent(ids_all.at[2:4], 2, is_end)
    sent(sized(count(blocks.at[0], slots_v)), 3, is_end)
    sent(sized(count(pick_send, dest_send)), 5, is_inner)


def kernel_body(tokens, norm_gain, router_weight, inner_weight, outer_weight, slot_tokens, slot_ids):
    del slot_ids
    tok_rows, width = tokens.shape
    experts_dev, cap_dev = slot_tokens.shape
    units = inner_weight.shape[2]
    dat_count = lax.axis_size("dat")
    slots = experts_dev * cap_dev
    wide = PAIR * LANES
    chunks = width // wide
    both = PAIR * tok_rows
    bf16, f32 = jnp.bfloat16, jnp.float32
    vmem = pl.BlockSpec(memory_space=pltpu.VMEM)
    hbm = pl.BlockSpec(memory_space=pltpu.HBM)
    dma = pltpu.SemaphoreType.DMA

    def buffer(*shape, kind=bf16):
        return pltpu.VMEM(shape, kind)

    return pl.pallas_call(
        moe_kernel,
        out_shape=jax.ShapeDtypeStruct((tok_rows, width), bf16),
        in_specs=[hbm] * 6,
        out_specs=vmem,
        scratch_shapes=[
            buffer(tok_rows, width),
            buffer(1, width, kind=f32),
            buffer(experts_dev, width),
            buffer(experts_dev, cap_dev, kind=jnp.int32),
            buffer(experts_dev, width, units),
            buffer(experts_dev, units, width),
            buffer(LINE, experts_dev, cap_dev, kind=jnp.int32),
            buffer(PAIR * slots, LINE * both),
            buffer(LINE * both, PAIR * slots),
            buffer(PAIR * slots, (LINE - 1) * both),
            buffer((LINE - 1) * both, PAIR * slots),
            buffer(chunks, LINE, PAIR, tok_rows, LANES),
            buffer(chunks, tok_rows, LANES),
            buffer(chunks, PAIR, experts_dev, cap_dev, LANES),
            buffer(chunks, PAIR, experts_dev, cap_dev, LANES),
            buffer(chunks, experts_dev, cap_dev, LANES),
            buffer(PAIR * chunks, experts_dev, dat_count * cap_dev, LANES),
            buffer(experts_dev, dat_count * cap_dev, units, kind=f32),
            buffer(experts_dev, dat_count * cap_dev, units),
            buffer(experts_dev, cap_dev, 1, kind=f32),
            buffer(chunks, PAIR, PAIR, experts_dev, cap_dev, wide),
            buffer(chunks, PAIR, experts_dev, cap_dev, wide),
            buffer(chunks, experts_dev, cap_dev, wide),
            buffer(chunks, experts_dev, cap_dev, wide),
            buffer(chunks, experts_dev, cap_dev, wide, kind=f32),
            buffer(chunks, experts_dev, cap_dev, LANES),
            buffer(chunks, PAIR, experts_dev, cap_dev, LANES),
            buffer(chunks, PAIR, experts_dev, cap_dev, LANES),
            buffer(chunks, both, LANES, kind=f32),
            buffer(chunks, LINE - 1, PAIR, tok_rows, LANES),
            buffer(chunks, 2, PAIR, tok_rows, LANES),
            buffer(chunks, tok_rows, LANES),
            buffer(chunks, tok_rows, LANES),
            buffer(chunks, tok_rows, LANES, kind=f32),
            dma((6,)),
            dma((5,)),
            dma((2,)),
            dma((chunks,)),
            dma((chunks,)),
            dma((chunks,)),
            dma((chunks, PAIR, PARTS)),
            dma((chunks, PARTS)),
            dma((chunks, PAIR, PARTS)),
            dma((chunks - 1 + PARTS,)),
            dma((chunks - 1 + PARTS,)),
            dma((chunks, PARTS)),
            dma((chunks, PARTS)),
            dma((chunks,)),
            dma((chunks,)),
            dma((chunks, PAIR)),
            dma((chunks,)),
        ],
        compiler_params=pltpu.CompilerParams(
            collective_id=0, has_side_effects=True, vmem_limit_bytes=48 * 1024 * 1024
        ),
    )(
        *(
            pltpu.with_memory_space_constraint(array, pltpu.HBM)
            for array in (tokens, norm_gain.reshape(1, width), router_weight.T, slot_tokens)
        ),
        inner_weight,
        outer_weight,
    )


def solution(mesh):
    fits = mesh.shape["dat"] == PAIR * PAIR and mesh.shape["exp"] == PAIR * LINE
    chosen = kernel_body if fits else body
    in_specs = (
        P(("exp", "dat"), None),
        P(),
        P(None, "exp"),
        P("exp", None, "dat"),
        P("exp", "dat", None),
        P("exp", "dat"),
        P(("exp", "dat"), None),
    )
    out_specs = P(("exp", "dat"), None)
    return jax.shard_map(chosen, mesh=mesh, in_specs=in_specs, out_specs=out_specs, check_vma=False)
```

```python
import jax
import jax.numpy as jnp
from jax import lax
from jax.experimental import pallas as pl
from jax.experimental.pallas import tpu as pltpu
from jax.sharding import PartitionSpec as P

EPSILON = 1e-06


def normalize(tokens, norm_gain):
    values = tokens.astype(jnp.float32)
    scale = lax.rsqrt(jnp.mean(values * values, axis=-1, keepdims=True) + EPSILON)
    return (values * scale * norm_gain).astype(jnp.bfloat16)


def owner_places(slot_ids, experts_dev, capacity, bucket):
    flat_ids = slot_ids.reshape(-1)
    source = flat_ids // capacity // experts_dev
    before = (source[:, None] == source[None, :]) & (flat_ids[None, :] < flat_ids[:, None])
    ranks_in = jnp.sum(before.astype(jnp.int32), axis=1)
    return (source * bucket + ranks_in).reshape(slot_ids.shape)


def expert_places(token_ids, slot_keys, tok_rows, dat_count, bucket):
    owner_of = token_ids // (tok_rows * dat_count)
    before = (owner_of[:, None] == owner_of[None, :]) & (slot_keys[None, :] < slot_keys[:, None])
    ranks_in = jnp.sum(before.astype(jnp.int32), axis=1)
    return owner_of * bucket + ranks_in


def body(tokens, norm_gain, router_weight, inner_weight, outer_weight, slot_tokens, slot_ids):
    exp_count = lax.axis_size("exp")
    dat_count = lax.axis_size("dat")
    tok_rows, width = tokens.shape
    experts_dev, cap_dev = slot_tokens.shape
    bucket = 6 * tok_rows // exp_count
    normed = normalize(tokens, norm_gain)
    picked = slot_tokens.T.reshape(-1)
    expert_iota = lax.broadcasted_iota(jnp.int32, (cap_dev, experts_dev), 1)
    column_iota = lax.broadcasted_iota(jnp.int32, (cap_dev, experts_dev), 0)
    slot_keys = (expert_iota * cap_dev + column_iota).reshape(-1)
    senders = expert_places(picked, slot_keys, tok_rows, dat_count, bucket)
    receivers = owner_places(slot_ids, experts_dev, cap_dev * dat_count, bucket)
    lookup = jnp.any(
        lax.broadcasted_iota(jnp.int32, (exp_count * bucket, 1, 1), 0) == receivers[None], axis=2
    )
    outgoing = jnp.dot(lookup.astype(jnp.bfloat16), normed, preferred_element_type=jnp.float32)
    outgoing = outgoing.astype(jnp.bfloat16).reshape(exp_count, bucket, width)
    arrived = lax.all_to_all(outgoing, "exp", split_axis=0, concat_axis=0, tiled=True).reshape(
        exp_count * bucket, width
    )
    gathered_rows = jnp.take(arrived, senders, axis=0)
    gathered_rows = gathered_rows.reshape(cap_dev, experts_dev, width)
    gate_score = jax.nn.sigmoid(
        jnp.einsum("ced,de->ce", gathered_rows, router_weight, preferred_element_type=jnp.float32)
    )
    inner = jnp.einsum(
        "ced,edf->cef",
        lax.all_gather(gathered_rows, "dat", axis=0, tiled=True),
        inner_weight,
        preferred_element_type=jnp.float32,
    )
    hidden = jax.nn.relu(inner).astype(jnp.bfloat16)
    expert_out = lax.psum_scatter(
        jnp.einsum("cef,efd->ced", hidden, outer_weight, preferred_element_type=jnp.float32).astype(
            jnp.bfloat16
        ),
        "dat",
        scatter_dimension=0,
        tiled=True,
    ).astype(jnp.float32)
    weighted = (gate_score[:, :, None] * expert_out).astype(jnp.bfloat16).reshape(-1, width)
    placing = lax.broadcasted_iota(jnp.int32, (exp_count * bucket, 1), 0) == senders[None, :]
    returning = jnp.dot(placing.astype(jnp.bfloat16), weighted, preferred_element_type=jnp.float32)
    returning = returning.astype(jnp.bfloat16).reshape(exp_count, bucket, width)
    came_back = lax.all_to_all(returning, "exp", split_axis=0, concat_axis=0, tiled=True).reshape(
        exp_count * bucket, width
    )
    combine_table = jnp.sum(
        (
            lax.broadcasted_iota(jnp.int32, (1, 1, exp_count * bucket), 2) == receivers[:, :, None]
        ).astype(jnp.float32),
        axis=1,
    )
    combined = jnp.dot(
        combine_table.astype(jnp.bfloat16), came_back, preferred_element_type=jnp.float32
    )
    return (tokens.astype(jnp.float32) + combined).astype(jnp.bfloat16)


MESH = pl.DeviceIdType.MESH
PAIR = 2
LINE = 4
LANES = 128
PARTS = 2
SENT_BY = {1: 1, 2: 2, 3: 3, 13: 3, 5: 4, 14: 4}
FIRST_AT = (9.6, 11.3, 14.5, 16.8)
RELAY_AT = (5.65, 8.45, 11.25, 12.4)
CROSS_IN = (-5.5, -5.4, -2.6, -1.9)


def moe_kernel(
    tokens_hbm, gain_hbm, router_hbm, ids_hbm, inner_hbm, outer_hbm, out_ref,
    tokens_ref, gain_ref, router_ref, ids_ref, inner_v, outer_v, ids_all, pick_own, place_own, pick_far, place_far,
    blocks, cross, pick_send, pick_recv, swap_send, rows, sums, hidden, gate,
    parts, core_recv, y_send, y_recv, kept, give, slots_v, raw, dense, dest_send, dest_recv,
    last_send, last_recv, last_own,
    w_sem, out_sem, ids_sem, x_sem, near_sem, far_sem, pick_sem, swap_sem, y_sem, c_sem, cr_sem,
    rc_sem, ry_sem, rx_sem, raw_sem, dest_sem, last_sem,
):
    chunks = blocks.shape[0]
    tok_rows = tokens_ref.shape[0]
    experts_dev, cap_dev = ids_ref.shape
    slots = experts_dev * cap_dev
    both = PAIR * tok_rows
    wide = PAIR * LANES
    pair_e = experts_dev // PARTS
    bf16, f32 = jnp.bfloat16, jnp.float32
    exp = lax.axis_index("exp")
    dat = lax.axis_index("dat")
    dat_count = lax.axis_size("dat")
    z, x = exp // PAIR, exp % PAIR
    y, c = dat // PAIR, dat % PAIR
    half = z // PAIR
    spot = z + half * (LINE - 1 - 2 * z)
    is_end = spot == 0
    is_inner = spot == 1

    def line_z(q):
        return q + half * (LINE - 1 - 2 * q)

    near = (line_z(1 - spot) * PAIR + x, dat)
    far_inner = (line_z(2) * PAIR + x, dat)
    far_end = (line_z(3) * PAIR + x, dat)
    x_peer = (exp + 1 - 2 * x, dat)
    y_peer = (exp, dat + PAIR - 2 * PAIR * y)
    c_peer = (exp, dat + 1 - 2 * c)
    near_diag = (line_z(1 - spot) * PAIR + 1 - x, dat)
    far_diag = (line_z(2) * PAIR + 1 - x, dat)
    far_end_diag = (line_z(3) * PAIR + 1 - x, dat)
    xy_diag = (exp + 1 - 2 * x, dat + PAIR - 2 * PAIR * y)
    last = chunks - 1

    def copy_to(src, dst, stage, sems, where, peer):
        return pltpu.make_async_remote_copy(
            src_ref=src, dst_ref=dst, send_sem=out_sem.at[SENT_BY.get(stage, 0)],
            recv_sem=sems.at[where], device_id=peer, device_id_type=MESH,
        )

    def send(copy, cond=None):
        if cond is None:
            copy.start()
        else:
            pl.when(cond)(copy.start)

    loads = []
    for e in range(experts_dev):
        loads.append(pltpu.make_async_copy(inner_hbm.at[e], inner_v.at[e], w_sem.at[0]))
    for e in range(experts_dev):
        loads.append(pltpu.make_async_copy(outer_hbm.at[e], outer_v.at[e], w_sem.at[1]))
    inner_load = pltpu.make_async_copy(inner_hbm, inner_v, w_sem.at[0])
    outer_load = pltpu.make_async_copy(outer_hbm, outer_v, w_sem.at[1])

    barrier = pltpu.get_barrier_semaphore()
    for peer in (near, near_diag, far_inner, far_diag, x_peer, y_peer, xy_diag, c_peer):
        pl.semaphore_signal(barrier, inc=1, device_id=peer, device_id_type=MESH)

    @pl.when(is_inner)
    def _():
        for peer in (far_end, far_end_diag):
            pl.semaphore_signal(barrier, inc=1, device_id=peer, device_id_type=MESH)

    smalls = []
    for i, (src, dst) in enumerate(
        ((ids_hbm, ids_ref), (tokens_hbm, tokens_ref), (gain_hbm, gain_ref), (router_hbm, router_ref))
    ):
        smalls.append(pltpu.make_async_copy(src, dst, w_sem.at[2 + i]))
        smalls[i].start()
    for load in loads:
        load.start()
    smalls[1].wait()
    smalls[2].wait()

    values = tokens_ref[...].astype(f32)
    scale = lax.rsqrt(jnp.mean(values * values, axis=-1, keepdims=True) + EPSILON)
    normed = values * scale * gain_ref[...]

    def split(value):
        low, high = value[..., :LANES], value[..., LANES:]
        return jnp.where(x == 0, low, high), jnp.where(x == 0, high, low)

    for k in range(chunks):
        own, other = split(normed[:, k * wide : (k + 1) * wide])
        blocks[k, spot, 0] = own.astype(bf16)
        cross[k] = other.astype(bf16)

    def one_hots(ids, side, pick, place, first):
        row = jnp.concatenate([ids[e : e + 1, :] for e in range(experts_dev)], axis=1)
        column = jnp.broadcast_to(row, (LANES, slots)).T
        lane = lax.broadcasted_iota(jnp.int32, (slots, tok_rows), 1)
        line = lax.broadcasted_iota(jnp.int32, (tok_rows, slots), 0)
        at = slice(side * slots, (side + 1) * slots)
        for q in range(first, LINE):
            for xr in range(PAIR):
                x_of = x if xr == 0 else 1 - x
                base = ((line_z(q) * PAIR + x_of) * dat_count + dat) * tok_rows
                start = ((q - first) * PAIR + xr) * tok_rows
                span = slice(start, start + tok_rows)
                pick[at, span] = (column == lane + base).astype(f32).astype(bf16)
                place[span, at] = (row == line + base).astype(f32).astype(bf16)

    smalls[0].wait()

    pl.semaphore_wait(barrier, 8 + 2 * is_inner.astype(jnp.int32))

    def cross_copy(k):
        return copy_to(cross.at[k], blocks.at[k, spot, 1], 0, x_sem, (k,), x_peer)

    ids_x = copy_to(ids_ref, ids_all.at[1], 1, ids_sem, (0,), x_peer)
    ids_near = copy_to(ids_ref, ids_all.at[2], 2, ids_sem, (1,), near)
    ids_diag = copy_to(ids_ref, ids_all.at[3], 2, ids_sem, (1,), near_diag)
    ids_both = copy_to(ids_all.at[2:4], ids_all.at[2:4], 2, ids_sem, (1,), near)

    def near_copy(k, xr):
        ref = blocks.at[k, 0, xr]
        return copy_to(ref, ref, 3, near_sem, (k,), near)

    def far_copy(k, xr):
        return copy_to(blocks.at[k, spot, xr], blocks.at[k, 3 - spot, xr], 4, far_sem, (k,), far_inner)

    def block_send(k, xr):
        send(far_copy(k, xr))
        send(near_copy(k, xr), is_end)

    def diag_send(k):
        send(copy_to(cross.at[k], blocks.at[k, 3 - spot, 1], 4, far_sem, (k,), far_diag))
        send(copy_to(cross.at[k], blocks.at[k, 0, 1], 3, near_sem, (k,), near_diag), is_end)

    send(ids_x)
    send(ids_near, is_end)
    send(ids_diag, is_end)
    send(cross_copy(0))
    diag_send(0)
    block_send(0, 0)
    send(cross_copy(1))
    block_send(1, 0)
    block_send(2, 0)
    for k in range(2, chunks):
        send(cross_copy(k))

    def stage_cross_in(k):
        cross_copy(k).wait_recv()
        if k > 0:
            block_send(k, 1)
        if k == 1:
            for j in range(3, chunks):
                block_send(j, 0)

    def stage_ids():
        one_hots(ids_ref, 0, pick_own, place_own, 0)
        ids_x.wait_recv()
        one_hots(ids_all.at[1], 1, pick_own, place_own, 0)

        @pl.when(is_inner)
        def _():
            ids_both.wait_recv()
            one_hots(ids_all.at[2], 0, pick_far, place_far, 1)
            one_hots(ids_all.at[3], 1, pick_far, place_far, 1)

    def pair(p):
        return slice(p * pair_e, (p + 1) * pair_e)

    def own_rows(k, rel, p, of_dat):
        feature = k * PAIR + (x if rel == 0 else 1 - x)
        at = pl.ds(pl.multiple_of(of_dat * cap_dev, cap_dev), cap_dev)
        return rows.at[feature, pair(p), at]

    def late_at(k, p):
        return (k + p if k == last else k,)

    def dat_at(of_dat):
        return pl.ds(pl.multiple_of(of_dat * cap_dev, cap_dev), cap_dev)

    def pick_copy(k, xr, p):
        return copy_to(
            pick_send.at[k, xr, pair(p)], pick_recv.at[k, xr, pair(p)], 5, pick_sem, (k, xr, p), near
        )

    def swap_copy(k, p):
        return copy_to(
            swap_send.at[k, pair(p)], own_rows(k, 0, p, dat), 6, swap_sem, (k, p), x_peer
        )

    def far_swap(k, p):
        return copy_to(
            swap_send.at[k, pair(p)], own_rows(k, 0, p, dat), 7, y_sem, (k, 1, p), xy_diag
        )

    def y_copy(k, rel, p, of_dat):
        ref = own_rows(k, rel, p, of_dat)
        return copy_to(ref, ref, 7, y_sem, (k, rel, p), y_peer)

    def c_copy(k, rel, p, of_dat):
        ref = own_rows(k, rel, p, of_dat)
        return copy_to(ref, ref, 8, c_sem, late_at(k, p), c_peer)

    def relay_copy(k, rel, p, of_dat):
        ref = own_rows(k, rel, p, of_dat)
        return copy_to(ref, ref, 9, cr_sem, late_at(k, p), c_peer)

    def both_rows(k, p, of_dat):
        parts_at = pair(p) if k == last else slice(0, experts_dev)
        return rows.at[k * PAIR : (k + 1) * PAIR, parts_at, dat_at(of_dat)]

    dat_y = dat + PAIR - 2 * PAIR * y
    dat_c = dat + 1 - 2 * c
    dat_yc = dat_y + 1 - 2 * c

    def by_part(value):
        size = pair_e * cap_dev
        return [
            value[p * size : (p + 1) * size].reshape(pair_e, cap_dev, LANES) for p in range(PARTS)
        ]

    def sides(k):
        return (1, 0) if k + 1 == chunks else (0, 1)

    def stage_far_pick(k):
        @pl.when(is_inner)
        def _():
            near_all, far_all = blocks.at[k, 0], blocks.at[k, 2:4]
            copy_to(near_all, near_all, 3, near_sem, (k,), near).wait_recv()
            copy_to(far_all, far_all, 4, far_sem, (k,), far_inner).wait_recv()
            found = blocks[k].reshape(LINE * both, LANES)
            for xr in sides(k):
                at = slice(xr * slots, (xr + 1) * slots)
                got = jnp.dot(pick_far[at, :], found[both:], preferred_element_type=f32)
                got = by_part(got.astype(bf16))
                for p in range(PARTS):
                    pick_send[k, xr, pair(p)] = got[p]
                    pick_copy(k, xr, p).start()

    def hand_on(k, xr, p, value):
        if xr == 1:
            swap_send[k, pair(p)] = value
            swap_copy(k, p).start()
            far_swap(k, p).start()
        else:
            own_rows(k, 0, p, dat)[...] = value
            y_copy(k, 0, p, dat).start()
            c_copy(k, 0, p, dat).start()

    def stage_pick(k):
        @pl.when(is_inner)
        def _():
            found = blocks[k].reshape(LINE * both, LANES)
            for xr in (1, 0):
                at = slice(xr * slots, (xr + 1) * slots)
                got = jnp.dot(pick_own[at, :], found, preferred_element_type=f32)
                got = by_part(got.astype(bf16))
                for p in range(PARTS):
                    hand_on(k, xr, p, got[p])

        @pl.when(is_end)
        def _():
            found = blocks[k, 0].reshape(both, LANES)
            for xr in sides(k):
                at = slice(xr * slots, (xr + 1) * slots)
                got = by_part(jnp.dot(pick_own[at, :both], found, preferred_element_type=f32))
                for p in range(PARTS):
                    pick_copy(k, xr, p).wait_recv()
                    here = got[p] + pick_recv[k, xr, pair(p)].astype(f32)
                    hand_on(k, xr, p, here.astype(bf16))

    def stage_swap(k):
        for p in range(PARTS):
            ref = own_rows(k, 1, p, dat)
            copy_to(ref, ref, 6, swap_sem, (k, p), x_peer).wait_recv()
            send(c_copy(k, 1, p, dat))

    def stage_relay(k, rel):
        for p in range(PARTS):
            y_copy(k, rel, p, dat_y).wait_recv()
            send(relay_copy(k, rel, p, dat_y))

    def stage_first(k, p):
        for sems, stage, of_dat in ((c_sem, 8, dat_c), (cr_sem, 9, dat_yc)):
            if k == last or p == 0:
                ref = both_rows(k, p, of_dat)
                copy_to(ref, ref, stage, sems, late_at(k, p), c_peer).wait_recv()
        if k == 0 and p == 0:
            inner_load.wait()

        for e in range(p * pair_e, (p + 1) * pair_e):
            left = jnp.concatenate([rows[PAIR * k, e], rows[PAIR * k + 1, e]], axis=1)
            total = jnp.dot(left, inner_v[e, k * wide : (k + 1) * wide, :], preferred_element_type=f32)
            if k > 0:
                total += sums[e]
            if k + 1 < chunks:
                sums[e] = total
            else:
                hidden[e] = jnp.maximum(total, 0.0).astype(bf16)

    def core_copy(k, p):
        return copy_to(
            parts.at[k, :, 1 - c, pair(p)], core_recv.at[k, :, pair(p)], 10, rc_sem, (k, p), c_peer
        )

    def back_y(k, p):
        return copy_to(y_send.at[k, pair(p)], y_recv.at[k, pair(p)], 11, ry_sem, (k, p), y_peer)

    def back_x(k, p):
        return copy_to(give.at[k, pair(p)], slots_v.at[k, 1, pair(p)], 12, rx_sem, (k,), x_peer)

    def raw_copy(k, xr, p):
        return copy_to(
            slots_v.at[k, xr, pair(p)], raw.at[k, xr, pair(p)], 13, raw_sem, (k,), near
        )

    def dest_copy(k, j, xr, peer):
        return copy_to(
            dest_send.at[k, j, xr], dest_recv.at[k, min(j, 1), xr], 14, dest_sem, (k, xr), peer
        )

    def last_copy(k):
        return copy_to(last_send.at[k], last_recv.at[k], 15, last_sem, (k,), x_peer)

    def stage_second(k, p):
        if k == 0 and p == 0:
            outer_load.wait()
        for e in range(p * pair_e, (p + 1) * pair_e):
            part = jnp.dot(
                hidden[e], outer_v[e, :, k * wide : (k + 1) * wide], preferred_element_type=f32
            ).astype(bf16)
            for d in range(PAIR * PAIR):
                parts[k, d // PAIR, d % PAIR, e] = part[d * cap_dev : (d + 1) * cap_dev]
        send(core_copy(k, p))

    def stage_core(k, p):
        core_copy(k, p).wait_recv()
        theirs = parts[k, 1 - y, c, pair(p)].astype(f32) + core_recv[k, 1 - y, pair(p)].astype(f32)
        y_send[k, pair(p)] = theirs.astype(bf16)
        send(back_y(k, p))
        ours = parts[k, y, c, pair(p)].astype(f32) + core_recv[k, y, pair(p)].astype(f32)
        kept[k, pair(p)] = ours

    def gates():
        smalls[3].wait()
        at = pl.ds(pl.multiple_of(dat * cap_dev, cap_dev), cap_dev)
        for e in range(experts_dev):
            score = jnp.zeros((cap_dev, LANES), f32)
            for b in range(PAIR * chunks):
                weight = router_ref[e : e + 1, b * LANES : (b + 1) * LANES].astype(f32)
                score += rows[b, e, at].astype(f32) * weight
            gate[e] = jax.nn.sigmoid(jnp.sum(score, axis=-1, keepdims=True))

    def stage_weigh(k, p):
        back_y(k, p).wait_recv()
        summed = kept[k, pair(p)] + y_recv[k, pair(p)].astype(f32)
        own, other = split(gate[pair(p)] * summed)
        give[k, pair(p)] = other.astype(bf16)
        ref = raw.at[k, 1, pair(p)]
        send(copy_to(give.at[k, pair(p)], ref, 13, raw_sem, (k,), near_diag), is_end)
        send(back_x(k, p))
        slots_v[k, 0, pair(p)] = own.astype(bf16)
        send(raw_copy(k, 0, p), is_end)

    def stage_cross(k):
        ref = slots_v.at[k, 1]
        copy_to(ref, ref, 12, rx_sem, (k,), x_peer).wait_recv()

    def dest_out(k, j, total, peer, peer_diag):
        for xr in (1, 0):
            dest_send[k, j, xr] = total[xr * tok_rows : (xr + 1) * tok_rows].astype(bf16)
            if (k, j, xr) != (last - 1, 1, 0):
                dest_copy(k, j, xr, peer_diag if k == last and xr == 1 else peer).start()

    def last_out(k, total):
        last_send[k] = total.astype(bf16)
        last_copy(k).start()

    def stage_place(k):
        held = slots_v[k].reshape(PAIR * slots, LANES)

        @pl.when(is_inner)
        def _():
            dest_out(k, 0, jnp.dot(place_own[:both, :], held, preferred_element_type=f32), near, near_diag)

        at = pl.ds(pl.multiple_of(spot * both, both), both)
        total = jnp.dot(place_own[at, :], held, preferred_element_type=f32)
        dense[k] = total
        if k == last:

            @pl.when(is_end)
            def _():
                last_out(k, total[tok_rows:])

    def stage_far(k):
        @pl.when(is_inner)
        def _():
            held = slots_v[k].reshape(PAIR * slots, LANES)
            mine = jnp.dot(place_own[2 * both :, :], held, preferred_element_type=f32)
            copy_to(raw.at[k], raw.at[k], 13, raw_sem, (k,), near).wait_recv()
            ends = raw[k].reshape(PAIR * slots, LANES)
            theirs = jnp.dot(place_far[2 * both :, :], ends, preferred_element_type=f32)
            dest_out(k, 2, mine[both:] + theirs, far_end, far_end_diag)
            if k == last:
                dest_copy(k - 1, 1, 0, far_inner).start()
            theirs = jnp.dot(place_far[both : 2 * both, :], ends, preferred_element_type=f32)
            dest_out(k, 1, mine[:both] + theirs, far_inner, far_diag)
            total = dense[k] + jnp.dot(place_far[:both, :], ends, preferred_element_type=f32)
            dense[k] = total
            if k == last:
                last_out(k, total[tok_rows:])

    def arrived(k, xr, ref):
        copy_to(ref, ref, 14, dest_sem, (k, xr), near).wait_recv()

    def stage_total(k):
        def finish(total, xr):
            if xr == 1:
                last_out(k, total)
            else:
                last_own[k] = total

        where = (0,) if k == last else (1, 0)

        @pl.when(is_end)
        def _():
            for xr in where:
                arrived(k, xr, dest_recv.at[k, :, xr])
                held = dense[k, xr * tok_rows : (xr + 1) * tok_rows]
                finish(held + dest_recv[k, 0, xr].astype(f32) + dest_recv[k, 1, xr].astype(f32), xr)

        @pl.when(is_inner)
        def _():
            for xr in where:
                arrived(k, xr, dest_recv.at[k, 1, xr])
                held = dense[k, xr * tok_rows : (xr + 1) * tok_rows]
                finish(held + dest_recv[k, 1, xr].astype(f32), xr)

    def stage_last(k):
        def finish(own, other):
            cols = slice(k * wide, (k + 1) * wide)
            left, right = jnp.where(x == 0, own, other), jnp.where(x == 0, other, own)
            total = jnp.concatenate([left, right], axis=1)
            out_ref[:, cols] = (tokens_ref[:, cols].astype(f32) + total).astype(bf16)

        last_copy(k).wait_recv()
        own, other = last_own[k], last_recv[k].astype(f32)
        if k < last:
            finish(own, other)
            return

        @pl.when(is_end)
        def _():
            arrived(k, 1, dest_recv.at[k, :, 1])
            finish(own, other + dest_recv[k, 0, 1].astype(f32) + dest_recv[k, 1, 1].astype(f32))

        @pl.when(is_inner)
        def _():
            arrived(k, 1, dest_recv.at[k, 1, 1])
            finish(own, other + dest_recv[k, 1, 1].astype(f32))

    def run_first(k):
        for p in range(PARTS):
            stage_first(k, p)
            if k == last:
                stage_second(0, p)

    order = [(-6.0, stage_ids, ())]
    for k in range(chunks):
        order += [
            (CROSS_IN[k], stage_cross_in, (k,)),
            (2.8 * k - 2.65, stage_far_pick, (k,)),
            (2.8 * k, stage_pick, (k,)),
            (2.8 * k + 3.1, stage_swap, (k,)),
            (2.8 * k + 3.9, stage_relay, (k, 0)),
            (RELAY_AT[k], stage_relay, (k, 1)),
            (FIRST_AT[k], run_first, (k,)),
        ]
    for _, stage, where in sorted(order, key=lambda step: step[0]):
        stage(*where)

    pieces = [(k, p) for k in range(chunks) for p in range(PARTS)]
    for i in range(PARTS, len(pieces)):
        stage_second(*pieces[i])
        stage_core(*pieces[i - PARTS])
    gates()
    for i in range(len(pieces) - PARTS, len(pieces)):
        stage_core(*pieces[i])

    order = []
    for k in range(chunks):
        order += [
            (2 * k + 0.0, stage_weigh, (k, 0)),
            (2 * k + 1.0, stage_weigh, (k, 1)),
            (2 * k + 3.1, stage_cross, (k,)),
            (2 * k + 3.2, stage_place, (k,)),
            (2 * k + 6.05, stage_far, (k,)),
            (2 * k + 11.4, stage_total, (k,)),
            (2 * k + 15.6, stage_last, (k,)),
        ]
    for _, stage, where in sorted(order, key=lambda step: step[0]):
        stage(*where)

    def count(*refs):
        total = 0
        for ref in refs:
            size = 1
            for extent in ref.shape:
                size *= extent
            total += size
        return total

    def sent(ref, stage, cond=None):
        done = copy_to(ref, ref, stage, ids_sem, (0,), x_peer)
        if cond is None:
            done.wait_send()
        else:
            pl.when(cond)(done.wait_send)

    width, units = inner_v.shape[1], inner_v.shape[2]

    def sized(total):
        whole_e, lines = divmod(total, width * units)
        if lines == 0:
            return outer_v.at[0:whole_e]
        assert whole_e == 0 and lines % width == 0
        return outer_v.at[0, 0 : lines // width]

    own_all = rows.at[:, :, dat_at(dat)]
    half_parts = parts.at[:, :, 1 - c]
    always = count(cross, blocks.at[0], swap_send, own_all, own_all, own_all, half_parts)
    always += count(y_send, give, last_send)
    sent(sized(always), 0)
    sent(ids_ref, 1)
    sent(ids_all.at[2:4], 2, is_end)
    sent(sized(count(blocks.at[0], slots_v)), 3, is_end)
    sent(sized(count(pick_send, dest_send)), 5, is_inner)


def kernel_body(tokens, norm_gain, router_weight, inner_weight, outer_weight, slot_tokens, slot_ids):
    del slot_ids
    tok_rows, width = tokens.shape
    experts_dev, cap_dev = slot_tokens.shape
    units = inner_weight.shape[2]
    dat_count = lax.axis_size("dat")
    slots = experts_dev * cap_dev
    wide = PAIR * LANES
    chunks = width // wide
    both = PAIR * tok_rows
    bf16, f32 = jnp.bfloat16, jnp.float32
    vmem = pl.BlockSpec(memory_space=pltpu.VMEM)
    hbm = pl.BlockSpec(memory_space=pltpu.HBM)
    dma = pltpu.SemaphoreType.DMA

    def buffer(*shape, kind=bf16):
        return pltpu.VMEM(shape, kind)

    return pl.pallas_call(
        moe_kernel,
        out_shape=jax.ShapeDtypeStruct((tok_rows, width), bf16),
        in_specs=[hbm] * 6,
        out_specs=vmem,
        scratch_shapes=[
            buffer(tok_rows, width),
            buffer(1, width, kind=f32),
            buffer(experts_dev, width),
            buffer(experts_dev, cap_dev, kind=jnp.int32),
            buffer(experts_dev, width, units),
            buffer(experts_dev, units, width),
            buffer(LINE, experts_dev, cap_dev, kind=jnp.int32),
            buffer(PAIR * slots, LINE * both),
            buffer(LINE * both, PAIR * slots),
            buffer(PAIR * slots, (LINE - 1) * both),
            buffer((LINE - 1) * both, PAIR * slots),
            buffer(chunks, LINE, PAIR, tok_rows, LANES),
            buffer(chunks, tok_rows, LANES),
            buffer(chunks, PAIR, experts_dev, cap_dev, LANES),
            buffer(chunks, PAIR, experts_dev, cap_dev, LANES),
            buffer(chunks, experts_dev, cap_dev, LANES),
            buffer(PAIR * chunks, experts_dev, dat_count * cap_dev, LANES),
            buffer(experts_dev, dat_count * cap_dev, units, kind=f32),
            buffer(experts_dev, dat_count * cap_dev, units),
            buffer(experts_dev, cap_dev, 1, kind=f32),
            buffer(chunks, PAIR, PAIR, experts_dev, cap_dev, wide),
            buffer(chunks, PAIR, experts_dev, cap_dev, wide),
            buffer(chunks, experts_dev, cap_dev, wide),
            buffer(chunks, experts_dev, cap_dev, wide),
            buffer(chunks, experts_dev, cap_dev, wide, kind=f32),
            buffer(chunks, experts_dev, cap_dev, LANES),
            buffer(chunks, PAIR, experts_dev, cap_dev, LANES),
            buffer(chunks, PAIR, experts_dev, cap_dev, LANES),
            buffer(chunks, both, LANES, kind=f32),
            buffer(chunks, LINE - 1, PAIR, tok_rows, LANES),
            buffer(chunks, 2, PAIR, tok_rows, LANES),
            buffer(chunks, tok_rows, LANES),
            buffer(chunks, tok_rows, LANES),
            buffer(chunks, tok_rows, LANES, kind=f32),
            dma((6,)),
            dma((5,)),
            dma((2,)),
            dma((chunks,)),
            dma((chunks,)),
            dma((chunks,)),
            dma((chunks, PAIR, PARTS)),
            dma((chunks, PARTS)),
            dma((chunks, PAIR, PARTS)),
            dma((chunks - 1 + PARTS,)),
            dma((chunks - 1 + PARTS,)),
            dma((chunks, PARTS)),
            dma((chunks, PARTS)),
            dma((chunks,)),
            dma((chunks,)),
            dma((chunks, PAIR)),
            dma((chunks,)),
        ],
        compiler_params=pltpu.CompilerParams(
            collective_id=0, has_side_effects=True, vmem_limit_bytes=48 * 1024 * 1024
        ),
    )(
        *(
            pltpu.with_memory_space_constraint(array, pltpu.HBM)
            for array in (tokens, norm_gain.reshape(1, width), router_weight.T, slot_tokens)
        ),
        inner_weight,
        outer_weight,
    )


def solution(mesh):
    fits = mesh.shape["dat"] == PAIR * PAIR and mesh.shape["exp"] == PAIR * LINE
    chosen = kernel_body if fits else body
    in_specs = (
        P(("exp", "dat"), None),
        P(),
        P(None, "exp"),
        P("exp", None, "dat"),
        P("exp", "dat", None),
        P("exp", "dat"),
        P(("exp", "dat"), None),
    )
    out_specs = P(("exp", "dat"), None)
    return jax.shard_map(chosen, mesh=mesh, in_specs=in_specs, out_specs=out_specs, check_vma=False)
```
